256 devices in a mesh: mem: 32 (over x, z_lo, y), tile: 8 (over z_hi, core).
Axes of the slice: x: 4, y: 4, z: 8 (z_hi: 4, z_lo: 2; z = z_hi * 2 + z_lo), core: 2. Of those that a mesh axis runs over, the one named last changes fastest.
Arguments:
- starting_samples: float32 [512, 512, 512], P('mem', 'tile'), may hold values from -6 to 6
- transport_number_vertical: float32 [512, 512], P('tile'), may hold values from 0.1 to 0.35
- transport_number_horizontal: float32 [512, 512], P('tile'), may hold values from 0.1 to 0.35
- spreading_number: float32 [512, 512], P('tile'), may hold values from 0.01 to 0.07
- obs_value: float32 [8, 32, 128], P('tile'), may hold values from -6 to 6
- obs_error: float32 [8, 32, 128], P('tile'), may hold values from 0.002 to 0.05
- obs_index: int32 [8, 32, 128], P('tile'), may hold values from 0 to 1023
- loc_index: int32 [8, 32, 128], P('tile'), may hold values from 0 to 7
- loc_table: float32 [3, 8], replicated, may hold values from 0.2 to 1
Outputs:
- analysis: float32 [512, 512, 512], P('mem', 'tile')
The draws below stay inside these ranges and needn't reach their ends.
Inputs may be any that keep to these rules, and one draw needn't show every extreme that they name: Observation j of a patch lies in the patch's cell obs_index, cells numbered row by row, 16 to a row.
All inputs are finite; a program needn't handle non-finite values.
Results may differ from the reference program's by a relative error of at most 0.0003.
Values sent between devices are 32-bit elements; how exact they have to be, the bound alone decides.
A program may use at most 128 MiB of HBM per device.

```python
import math
import jax
import jax.numpy as jnp
from jax import lax

ENSEMBLE_SIZE_N = 512
STRIP_HEIGHT = 64
BLOCK_WIDTH = 16
NOBS = 128
LEVELS = 8
PASSES = 6
NS_ITERS = 8
STRIP_TOTAL = 8
BLOCKS_ACROSS = 32
NX = 512
NY = 512
PATCH_CELLS = 1024


def place_ends(values, stream_key, smallest, top_value):
    index_at = [jax.random.randint(jax.random.fold_in(stream_key, axis), (), 0, length) for axis, length in enumerate(values.shape)]
    widest = values.shape.index(max(values.shape))
    next_to = index_at[:widest] + [(index_at[widest] + 1) % values.shape[widest]] + index_at[widest + 1:]
    return values.at[tuple(index_at)].set(smallest).at[tuple(next_to)].set(top_value)


def block_scale(key, dims, cuts, low, high):
    loudness = 1.0
    for axis_at, blocks in cuts:
        heights = jax.random.uniform(jax.random.fold_in(jax.random.fold_in(key, 6), axis_at), (blocks,), jnp.float32, low / len(cuts), high / len(cuts))
        loudness = loudness * jnp.repeat(jnp.exp(heights), dims[axis_at] // blocks).reshape((-1,) + (1,) * (len(dims) - 1 - axis_at))
    return loudness


def bell_draw(rng, extent, deviation, limit, split=(), kind=jnp.bfloat16):
    array = deviation * jax.random.normal(rng, extent, jnp.float32)
    if split:
        array = array * block_scale(rng, extent, split, -0.22, 0.18)
    return jnp.clip(array, -limit, limit).astype(kind)


def setup_inputs(seed: int = 0) -> dict:
    splits = jax.random.split(jax.random.key(seed), 10)
    starting_samples = bell_draw(splits[0], (ENSEMBLE_SIZE_N, NY, NX), 1.0, 6.0, ((0, 32), (1, 8)), jnp.float32)
    transport_number_vertical = jnp.clip(0.1 + 0.25 * jax.random.uniform(splits[1], (NY, NX), jnp.float32) ** block_scale(splits[1], (NY, NX), ((0, 8),), -0.2, 0.2), 0.1, 0.35)
    transport_number_horizontal = jnp.clip(0.1 + 0.25 * jax.random.uniform(splits[2], (NY, NX), jnp.float32) ** block_scale(splits[2], (NY, NX), ((0, 8),), -0.2, 0.2), 0.1, 0.35)
    spreading_number = jnp.clip(0.01 + 0.060000001 * jax.random.uniform(splits[3], (NY, NX), jnp.float32) ** block_scale(splits[3], (NY, NX), ((0, 8),), -0.2, 0.2), 0.01, 0.07)
    obs_value = bell_draw(splits[4], (STRIP_TOTAL, BLOCKS_ACROSS, NOBS), 1.0, 6.0, ((0, 8),), jnp.float32)
    obs_error = jnp.clip(jnp.exp(math.log(0.05) - 3.218876 * jax.random.uniform(splits[5], (STRIP_TOTAL, BLOCKS_ACROSS, NOBS), jnp.float32) ** block_scale(splits[5], (STRIP_TOTAL, BLOCKS_ACROSS, NOBS), ((0, 8),), -0.2, 0.2)), 0.002, 0.05)
    obs_index = place_ends(jax.random.randint(splits[6], (STRIP_TOTAL, BLOCKS_ACROSS, NOBS), 0, PATCH_CELLS), jax.random.fold_in(splits[6], 1), 0, PATCH_CELLS - 1).astype(jnp.int32)
    loc_index = place_ends(jax.random.randint(splits[7], (STRIP_TOTAL, BLOCKS_ACROSS, NOBS), 0, LEVELS), jax.random.fold_in(splits[7], 1), 0, LEVELS - 1).astype(jnp.int32)
    loc_table = jnp.clip(jnp.exp(jax.random.uniform(splits[8], (3, LEVELS), jnp.float32, math.log(0.2), math.log(1.0))), 0.2, 1.0)
    return {"starting_samples": starting_samples, "transport_number_vertical": transport_number_vertical, "transport_number_horizontal": transport_number_horizontal, "spreading_number": spreading_number, "obs_value": obs_value, "obs_error": obs_error, "obs_index": obs_index, "loc_index": loc_index, "loc_table": loc_table}


def advance(middle, northern, southern, speed_x, speed_y, mixing, roll_axis):
    western = jnp.roll(middle, 1, axis=roll_axis)
    eastern = jnp.roll(middle, -1, axis=roll_axis)
    return middle + speed_x * (western - middle) + speed_y * (northern - middle) + mixing * (northern + southern + western + eastern - 4.0 * middle)

def transform(members, observed, values, errors, levels, loc_table):
    ensemble_size = members.shape[0]
    center = lax.optimization_barrier(jnp.mean(members, axis=0))
    anomaly = members - center
    obs_mean = lax.optimization_barrier(jnp.mean(observed, axis=1))
    spread = observed - obs_mean[:, None, :]
    innovation = values - obs_mean
    onehot = (levels[:, :, None] == jnp.arange(loc_table.shape[1], dtype=jnp.int32)).astype(jnp.float32)
    weights = lax.optimization_barrier(jnp.sum(onehot * loc_table[:, None, :], axis=2))
    precision_obs = weights / errors
    stacked = jnp.transpose(spread, (1, 0, 2)).reshape(ensemble_size, -1)
    scaled_obs = precision_obs.reshape(-1)
    weighted_innov = (precision_obs * innovation).reshape(-1)
    identity = jnp.eye(ensemble_size, dtype=jnp.float32)
    gram_matrix = (ensemble_size - 1.0) * identity + jnp.dot(stacked * scaled_obs, stacked.T, precision=lax.Precision.HIGHEST)
    norm_scale = jnp.sqrt(jnp.sum(gram_matrix * gram_matrix))
    matrix = gram_matrix / norm_scale
    inverse_root = identity
    for repeat in range(NS_ITERS):
        factor = 1.5 * identity - 0.5 * jnp.dot(inverse_root, matrix, precision=lax.Precision.HIGHEST)
        matrix = jnp.dot(matrix, factor, precision=lax.Precision.HIGHEST)
        inverse_root = jnp.dot(factor, inverse_root, precision=lax.Precision.HIGHEST)
    obs_pull = jnp.dot(stacked, weighted_innov, precision=lax.Precision.HIGHEST)
    mean_weight = jnp.dot(inverse_root, jnp.dot(inverse_root, obs_pull, precision=lax.Precision.HIGHEST), precision=lax.Precision.HIGHEST) / norm_scale
    weight = jnp.sqrt((ensemble_size - 1.0) / norm_scale) * inverse_root + mean_weight[:, None]
    return center + jnp.dot(weight.T, anomaly, precision=lax.Precision.HIGHEST)

def sample_prediction(model_mesh_values, transport_number_vertical, transport_number_horizontal, spreading_number):
    for repeat in range(PASSES):
        northern = jnp.roll(model_mesh_values, 1, axis=0)
        southern = jnp.roll(model_mesh_values, -1, axis=0)
        model_mesh_values = advance(model_mesh_values, northern, southern, transport_number_vertical, transport_number_horizontal, spreading_number, 1)
    return model_mesh_values

def reference(starting_samples, transport_number_vertical, transport_number_horizontal, spreading_number, obs_value, obs_error, obs_index, loc_index, loc_table):
    predict_advance = lax.map(lambda sample_mesh_values: sample_prediction(sample_mesh_values, transport_number_vertical, transport_number_horizontal, spreading_number), starting_samples)
    row_in = obs_index // BLOCK_WIDTH
    col_in = obs_index % BLOCK_WIDTH
    entire_mesh_lines = jnp.arange(STRIP_TOTAL, dtype=jnp.int32)[:, None, None] * STRIP_HEIGHT + row_in
    domain_verticals = jnp.arange(BLOCKS_ACROSS, dtype=jnp.int32)[None, :, None] * BLOCK_WIDTH + col_in
    measured_at_all_sites = predict_advance[:, entire_mesh_lines, domain_verticals]
    block_sequence = predict_advance.reshape(ENSEMBLE_SIZE_N, STRIP_TOTAL, STRIP_HEIGHT, BLOCKS_ACROSS, BLOCK_WIDTH)
    zero_index = jnp.zeros((), jnp.int32)

    def one_patch(flat_index):
        tile_number = (flat_index // BLOCKS_ACROSS).astype(jnp.int32)
        block_number = (flat_index % BLOCKS_ACROSS).astype(jnp.int32)
        members = lax.dynamic_slice(block_sequence, (zero_index, tile_number, zero_index, block_number, zero_index), (ENSEMBLE_SIZE_N, 1, STRIP_HEIGHT, 1, BLOCK_WIDTH)).reshape(ENSEMBLE_SIZE_N, STRIP_HEIGHT * BLOCK_WIDTH)
        role_blocks = (block_number + jnp.arange(3, dtype=jnp.int32) - 1) % BLOCKS_ACROSS
        seen_values = jnp.transpose(measured_at_all_sites[:, tile_number][:, role_blocks], (1, 0, 2))
        values = obs_value[tile_number][role_blocks]
        errors = obs_error[tile_number][role_blocks]
        levels = loc_index[tile_number][role_blocks]
        return transform(members, seen_values, values, errors, levels, loc_table)
    result = lax.map(one_patch, jnp.arange(STRIP_TOTAL * BLOCKS_ACROSS, dtype=jnp.int32))
    result = result.reshape(STRIP_TOTAL, BLOCKS_ACROSS, ENSEMBLE_SIZE_N, STRIP_HEIGHT, BLOCK_WIDTH)
    return jnp.transpose(result, (2, 0, 3, 1, 4)).reshape(ENSEMBLE_SIZE_N, NY, NX)
```

```python
import functools

import jax
import jax.numpy as jnp
from jax import lax
from jax.experimental import pallas as pl
from jax.experimental.pallas import tpu as pltpu
from jax.sharding import PartitionSpec as P

PASSES = 6
NS_ITERS = 8
PAD = 8
ROWS = 64
COLS = 16
MESH = pl.DeviceIdType.MESH
VMEM_LIMIT = 62 * 1024 * 1024


def split(x):
    high = x.astype(jnp.bfloat16)
    low = (x - high.astype(jnp.float32)).astype(jnp.bfloat16)
    return high, low


def dot(a, b):
    return jnp.dot(a, b, preferred_element_type=jnp.float32)


def dot3(a_high, a_low, b_high, b_low):
    return dot(a_high, b_high) + (dot(a_high, b_low) + dot(a_low, b_high))


def exchange_groups(rows, group):
    rows = list(rows)
    for bit in range(3):
        step = 1 << bit
        keep = (group & step) == 0
        for i in range(8):
            if i & step:
                continue
            a, b = rows[i], rows[i + step]
            rows[i] = jnp.where(keep, a, pltpu.roll(b, COLS * step, 1))
            rows[i + step] = jnp.where(keep, pltpu.roll(a, 128 - COLS * step, 1), b)
    return rows


def main_kernel(
    field,
    coef_x,
    coef_y,
    coef_mix,
    obs_value,
    obs_error,
    obs_index,
    loc_index,
    loc_table,
    back,
    levels,
    raw,
    coef,
    packed,
    picked,
    members,
    seen,
    matrix,
    root,
    matrix_parts,
    root_parts,
    factor_parts,
    anomaly_parts,
    result,
    load_sem,
    halo_send,
    halo_recv,
    seen_send,
    seen_recv,
    patch_send,
    patch_recv,
    back_send,
    back_recv,
    *,
    parts,
    tiles,
):
    me = lax.axis_index("mem")
    tile = lax.axis_index("tile")
    own = field.shape[0]
    width = field.shape[2]
    size = own * parts
    cells = ROWS * COLS
    nobs = obs_value.shape[2]
    lane_tiles = width // 128
    below = lax.rem(tile + 1, tiles)
    above = lax.rem(tile + tiles - 1, tiles)

    def peer(k):
        return lax.rem(me + 11 * k, parts)

    def source(k):
        return lax.rem(me + 12 * parts - 11 * k, parts)

    loads = []
    for m in range(own):
        loads.append(
            pltpu.make_async_copy(
                field.at[m], levels.at[0, pl.ds(PAD, ROWS), m], load_sem.at[m]
            )
        )
    for i, ref in enumerate((coef_x, coef_y, coef_mix)):
        loads.append(
            pltpu.make_async_copy(ref, raw.at[i, pl.ds(PAD, ROWS)], load_sem.at[own + i])
        )
    for load in loads:
        load.start()

    barrier = pltpu.get_barrier_semaphore()

    def greet(k, carry):
        pl.semaphore_signal(barrier, inc=1, device_id=(peer(k), tile), device_id_type=MESH)
        return carry

    pl.semaphore_signal(barrier, inc=1, device_id=(me, below), device_id_type=MESH)
    pl.semaphore_signal(barrier, inc=1, device_id=(me, above), device_id_type=MESH)
    lax.fori_loop(1, parts, greet, 0)
    pl.semaphore_wait(barrier, parts + 1)
    for load in loads:
        load.wait()

    halo = []
    for number, (target, src, dst) in enumerate(
        (
            (below, PAD + ROWS - PASSES, PAD - PASSES),
            (above, PAD, PAD + ROWS),
        )
    ):
        halo.append(
            pltpu.make_async_remote_copy(
                src_ref=levels.at[0, pl.ds(src, PASSES)],
                dst_ref=levels.at[0, pl.ds(dst, PASSES)],
                send_sem=halo_send.at[number],
                recv_sem=halo_recv.at[number],
                device_id=(me, target),
                device_id_type=MESH,
            )
        )
    for number, (target, src, dst) in enumerate(
        ((below, ROWS, 0), (above, PAD, PAD + ROWS))
    ):
        halo.append(
            pltpu.make_async_remote_copy(
                src_ref=raw.at[:, pl.ds(src, PAD)],
                dst_ref=raw.at[:, pl.ds(dst, PAD)],
                send_sem=halo_send.at[2 + number],
                recv_sem=halo_recv.at[2 + number],
                device_id=(me, target),
                device_id_type=MESH,
            )
        )
    for copy in halo:
        copy.start()

    def widen(row, carry):
        sx = raw[0, pl.ds(row, 1), :]
        sy = raw[1, pl.ds(row, 1), :]
        mix = raw[2, pl.ds(row, 1), :]
        for i, value in enumerate((1.0 - sx - sy - 4.0 * mix, sx + mix, sy + mix, mix)):
            coef[i, row] = jnp.broadcast_to(value, (8, width))
        return carry

    def step(level, first, count):
        def one(i, carry):
            row = first + i
            for half in range(own // 8):
                at = pl.ds(8 * half, 8)
                middle = levels[level, row, at, :]
                north = levels[level, row - 1, at, :]
                south = levels[level, row + 1, at, :]
                west = pltpu.roll(middle, 1, 1)
                east = pltpu.roll(middle, width - 1, 1)
                levels[level + 1, row, at, :] = (
                    coef[0, row] * middle + coef[1, row] * west
                ) + (coef[2, row] * north + coef[3, row] * (south + east))
            return carry

        lax.fori_loop(0, count, one, 0, unroll=2)

    lax.fori_loop(PAD, PAD + ROWS, widen, 0)
    for k in range(1, PASSES):
        step(k - 1, PAD + k, ROWS - 2 * k)
    for copy in halo:
        copy.wait_recv()
    lax.fori_loop(PAD - PASSES, PAD, widen, 0)
    lax.fori_loop(PAD + ROWS, PAD + ROWS + PASSES, widen, 0)
    for k in range(1, PASSES):
        step(k - 1, PAD - PASSES + k, PASSES)
        step(k - 1, PAD + ROWS - k, PASSES)
    step(PASSES - 1, PAD, ROWS)

    group = lax.broadcasted_iota(jnp.int32, (8, 128), 1) // COLS

    def pack(g, carry):
        lanes = pl.ds(pl.multiple_of(g * 128, 128), 128)
        for half in range(own // 8):
            at = pl.ds(8 * half, 8)
            for block in range(lane_tiles):
                rows = [
                    levels[PASSES, PAD + 8 * g + r, at, pl.ds(128 * block, 128)]
                    for r in range(8)
                ]
                for p, value in enumerate(exchange_groups(rows, group)):
                    packed[8 * block + p, at, lanes] = value
        return carry

    lax.fori_loop(0, ROWS // 8, pack, 0)

    def pick(b, carry):
        index = jnp.broadcast_to(obs_index[0, pl.ds(b, 1), :], (8, nobs))
        lane = index % 128
        place = index // 128
        for half in range(own // 8):
            at = pl.ds(8 * half, 8)
            total = jnp.zeros((8, nobs), jnp.float32)
            for g in range(cells // 128):
                found = jnp.take_along_axis(
                    packed[b, at, pl.ds(128 * g, 128)], lane, axis=1, mode="promise_in_bounds"
                )
                total = jnp.where(place == g, found, total)
            picked[b + 1, at, :] = total
        return carry

    lax.fori_loop(0, parts, pick, 0)
    picked[0] = picked[parts]
    picked[parts + 1] = picked[1]

    mine = pl.ds(pl.multiple_of(own * me, own), own)

    def seen_copy(k):
        return pltpu.make_async_remote_copy(
            src_ref=picked.at[pl.ds(peer(k), 3)],
            dst_ref=seen.at[:, mine],
            send_sem=seen_send.at[k],
            recv_sem=seen_recv.at[me],
            device_id=(peer(k), tile),
            device_id_type=MESH,
        )

    def patch_copy(k):
        return pltpu.make_async_remote_copy(
            src_ref=packed.at[peer(k)],
            dst_ref=members.at[mine],
            send_sem=patch_send.at[k],
            recv_sem=patch_recv.at[me],
            device_id=(peer(k), tile),
            device_id_type=MESH,
        )

    def back_copy(k):
        rows = pl.ds(pl.multiple_of(own * peer(k), own), own)
        return pltpu.make_async_remote_copy(
            src_ref=result.at[rows],
            dst_ref=back.at[me],
            send_sem=back_send.at[k],
            recv_sem=back_recv.at[me],
            device_id=(peer(k), tile),
            device_id_type=MESH,
        )

    def start_all(make):
        def one(k, carry):
            make(k).start()
            return carry

        lax.fori_loop(1, parts, one, 0)

    def wait_send_all(make):
        def one(k, carry):
            make(k).wait_send()
            return carry

        lax.fori_loop(1, parts, one, 0)

    def wait_seen(k, carry):
        rows = pl.ds(pl.multiple_of(own * source(k), own), own)
        pltpu.make_async_remote_copy(
            src_ref=picked.at[pl.ds(0, 3)],
            dst_ref=seen.at[:, rows],
            send_sem=seen_send.at[k],
            recv_sem=seen_recv.at[source(k)],
            device_id=(peer(k), tile),
            device_id_type=MESH,
        ).wait_recv()
        return carry

    def wait_patch(k, carry):
        rows = pl.ds(pl.multiple_of(own * source(k), own), own)
        pltpu.make_async_remote_copy(
            src_ref=packed.at[0],
            dst_ref=members.at[rows],
            send_sem=patch_send.at[k],
            recv_sem=patch_recv.at[source(k)],
            device_id=(peer(k), tile),
            device_id_type=MESH,
        ).wait_recv()
        return carry

    def wait_back(k, carry):
        pltpu.make_async_remote_copy(
            src_ref=result.at[pl.ds(0, own)],
            dst_ref=back.at[source(k)],
            send_sem=back_send.at[k],
            recv_sem=back_recv.at[source(k)],
            device_id=(peer(k), tile),
            device_id_type=MESH,
        ).wait_recv()
        return carry

    start_all(seen_copy)
    start_all(patch_copy)
    for role in range(3):
        seen[role, mine, :] = picked[me + role]
    members[mine, :] = packed[me]
    lax.fori_loop(1, parts, wait_seen, 0)

    row_id = lax.broadcasted_iota(jnp.int32, (size, size), 0)
    column_id = lax.broadcasted_iota(jnp.int32, (size, size), 1)
    diagonal = row_id == column_id
    gram = jnp.where(diagonal, size - 1.0, 0.0)
    pull = jnp.zeros((size, 1), jnp.float32)
    for role in range(3):
        patch = lax.rem(me + role + parts - 1, parts)
        value = obs_value[0, pl.ds(patch, 1), :]
        error = obs_error[0, pl.ds(patch, 1), :]
        level = loc_index[0, pl.ds(patch, 1), :]
        weight = jnp.zeros_like(value)
        for i in range(loc_table.shape[1]):
            weight = weight + jnp.where(level == i, loc_table[role, i], 0.0)
        precision = weight / error
        observed = seen[role]
        obs_mean = jnp.sum(observed, axis=0, keepdims=True) * (1.0 / size)
        spread = observed - obs_mean
        pull = pull + jnp.sum(
            spread * (precision * (value - obs_mean)), axis=1, keepdims=True
        )
        left_high, left_low = split(spread * precision)
        right_high, right_low = split(spread)
        gram = gram + sum(
            lax.dot_general(
                a, b, (((1,), (1,)), ((), ())), preferred_element_type=jnp.float32
            )
            for a, b in (
                (left_high, right_high),
                (left_high, right_low),
                (left_low, right_high),
                (left_low, right_low),
            )
        )
    square = jnp.sum(jnp.sum(gram * gram, axis=0, keepdims=True), axis=1, keepdims=True)
    inverse_scale = lax.rsqrt(square)
    inverse_scale = 1.0 / jnp.sqrt(square)

    def put(parts_ref, value):
        high, low = split(value)
        parts_ref[0] = high
        parts_ref[1] = low

    def product(a, b):
        return dot3(a[0], a[1], b[0], b[1])

    scaled = gram * inverse_scale
    put(matrix_parts, scaled)
    factor = jnp.where(diagonal, 1.5, 0.0) - 0.5 * scaled
    put(factor_parts, factor)
    put(root_parts, factor)
    put(matrix_parts, product(matrix_parts, factor_parts))

    def iterate(i, carry):
        put(
            factor_parts,
            jnp.where(diagonal, 1.5, 0.0) - 0.5 * product(root_parts, matrix_parts),
        )
        put(matrix_parts, product(matrix_parts, factor_parts))
        put(root_parts, product(factor_parts, root_parts))
        return carry

    lax.fori_loop(0, NS_ITERS - 2, iterate, 0)
    put(
        factor_parts,
        jnp.where(diagonal, 1.5, 0.0) - 0.5 * product(root_parts, matrix_parts),
    )
    root[...] = product(factor_parts, root_parts)

    pull_row = jnp.sum(jnp.where(diagonal, pull, 0.0), axis=0, keepdims=True)
    once = jnp.sum(root[...] * pull_row, axis=1, keepdims=True)
    mean_weight = jnp.sum(root[...] * once, axis=0, keepdims=True) * inverse_scale
    put(root_parts, jnp.sqrt((size - 1.0) * inverse_scale) * root[...] + mean_weight)

    lax.fori_loop(1, parts, wait_patch, 0)
    chunk = 256
    for c in range(cells // chunk):
        lanes = pl.ds(chunk * c, chunk)
        block = members[:, lanes]
        center = jnp.sum(block, axis=0, keepdims=True) * (1.0 / size)
        high, low = split(block - center)
        result[:, lanes] = center + dot3(root_parts[0], root_parts[1], high, low)
    start_all(back_copy)
    back[me] = result[mine, :]
    lax.fori_loop(1, parts, wait_back, 0)
    for copy in halo:
        copy.wait_send()
    wait_send_all(seen_copy)
    wait_send_all(patch_copy)
    wait_send_all(back_copy)


def unpack_kernel(back, out, rows_ref, sem):
    own = back.shape[1]
    lane_tiles = rows_ref.shape[2] // 128
    group = lax.broadcasted_iota(jnp.int32, (8, 128), 1) // COLS

    def unpack(g, carry):
        lanes = pl.ds(pl.multiple_of(g * 128, 128), 128)
        for half in range(own // 8):
            at = pl.ds(8 * half, 8)
            for block in range(lane_tiles):
                values = [back[8 * block + p, at, lanes] for p in range(8)]
                for r, value in enumerate(exchange_groups(values, group)):
                    rows_ref[8 * g + r, at, pl.ds(128 * block, 128)] = value
        return carry

    lax.fori_loop(0, ROWS // 8, unpack, 0)
    copies = [
        pltpu.make_async_copy(rows_ref.at[:, m], out.at[m], sem.at[m]) for m in range(own)
    ]
    for copy in copies:
        copy.start()
    for copy in copies:
        copy.wait()


def body(*args, parts, tiles):
    field = args[0]
    own, _, width = field.shape
    size = own * parts
    cells = ROWS * COLS
    nobs = args[4].shape[2]
    f32 = jnp.float32
    dma = pltpu.SemaphoreType.DMA
    hbm = pl.BlockSpec(memory_space=pl.ANY)
    vmem = pl.BlockSpec(memory_space=pltpu.VMEM)
    smem = pl.BlockSpec(memory_space=pltpu.SMEM)
    tall = ROWS + 2 * PAD
    pair = pltpu.VMEM((2, size, size), jnp.bfloat16)
    back = pl.pallas_call(
        functools.partial(main_kernel, parts=parts, tiles=tiles),
        out_shape=jax.ShapeDtypeStruct((parts, own, cells), f32),
        in_specs=[hbm] * 4 + [vmem] * 4 + [smem],
        out_specs=vmem,
        scratch_shapes=[
            pltpu.VMEM((PASSES + 1, tall, own, width), f32),
            pltpu.VMEM((3, tall, width), f32),
            pltpu.VMEM((4, tall, 8, width), f32),
            pltpu.VMEM((parts, own, cells), f32),
            pltpu.VMEM((parts + 2, own, nobs), f32),
            pltpu.VMEM((size, cells), f32),
            pltpu.VMEM((3, size, nobs), f32),
            pltpu.VMEM((8, 128), f32),
            pltpu.VMEM((size, size), f32),
            pair,
            pair,
            pair,
            pltpu.VMEM((8, 128), f32),
            pltpu.VMEM((size, cells), f32),
            dma((own + 3,)),
            dma((4,)),
            dma((4,)),
            dma((parts,)),
            dma((parts,)),
            dma((parts,)),
            dma((parts,)),
            dma((parts,)),
            dma((parts,)),
        ],
        compiler_params=pltpu.CompilerParams(
            collective_id=0, has_side_effects=True, vmem_limit_bytes=VMEM_LIMIT
        ),
        name="forecast_and_analysis",
    )(*args)
    return pl.pallas_call(
        unpack_kernel,
        out_shape=jax.ShapeDtypeStruct(field.shape, f32),
        in_specs=[vmem],
        out_specs=hbm,
        scratch_shapes=[pltpu.VMEM((ROWS, own, width), f32), dma((own,))],
        name="unpack",
    )(back)


def solution(mesh):
    parts, tiles = mesh.shape["mem"], mesh.shape["tile"]
    in_specs = (
        P("mem", "tile", None),
        P("tile", None),
        P("tile", None),
        P("tile", None),
        P("tile", None, None),
        P("tile", None, None),
        P("tile", None, None),
        P("tile", None, None),
        P(),
    )
    return jax.shard_map(
        functools.partial(body, parts=parts, tiles=tiles),
        mesh=mesh,
        in_specs=in_specs,
        out_specs=P("mem", "tile", None),
        check_vma=False,
    )
```

```python
import functools

import jax
import jax.numpy as jnp
from jax import lax
from jax.experimental import pallas as pl
from jax.experimental.pallas import tpu as pltpu
from jax.sharding import PartitionSpec as P

PASSES = 6
NS_ITERS = 8
PAD = 8
ROWS = 64
COLS = 16
UNROLL = 8
CHUNKS = 2
MESH = pl.DeviceIdType.MESH
VMEM_LIMIT = 62 * 1024 * 1024


def split(x):
    high = x.astype(jnp.bfloat16)
    low = (x - high.astype(jnp.float32)).astype(jnp.bfloat16)
    return high, low


def dot(a, b):
    return jnp.dot(a, b, preferred_element_type=jnp.float32)


def dot3(a_high, a_low, b_high, b_low):
    return dot(a_high, b_high) + (dot(a_high, b_low) + dot(a_low, b_high))


def exchange_groups(rows, group):
    rows = list(rows)
    for bit in range(3):
        step = 1 << bit
        keep = (group & step) == 0
        for i in range(8):
            if i & step:
                continue
            a, b = rows[i], rows[i + step]
            rows[i] = jnp.where(keep, a, pltpu.roll(b, COLS * step, 1))
            rows[i + step] = jnp.where(keep, pltpu.roll(a, 128 - COLS * step, 1), b)
    return rows


def main_kernel(
    field,
    coef_x,
    coef_y,
    coef_mix,
    obs_value,
    obs_error,
    obs_index,
    loc_index,
    loc_table,
    out,
    levels,
    raw,
    coef,
    packed,
    picked,
    members,
    seen,
    root,
    matrix_parts,
    root_parts,
    factor_parts,
    back,
    result,
    load_sem,
    out_sem,
    news_sem,
    halo_send,
    halo_recv,
    seen_send,
    seen_recv,
    patch_send,
    patch_recv,
    back_send,
    back_recv,
    *,
    parts,
    tiles,
):
    me = lax.axis_index("mem")
    tile = lax.axis_index("tile")
    own = field.shape[0]
    width = field.shape[2]
    size = own * parts
    cells = ROWS * COLS
    nobs = obs_value.shape[2]
    lane_tiles = width // 128
    below = lax.rem(tile + 1, tiles)
    above = lax.rem(tile + tiles - 1, tiles)

    def peer(k):
        return lax.rem(me + 11 * k, parts)

    def source(k):
        return lax.rem(me + 12 * parts - 11 * k, parts)

    loads = []
    for m in range(own):
        loads.append(
            pltpu.make_async_copy(
                field.at[m], levels.at[0, pl.ds(PAD, ROWS), m], load_sem.at[m]
            )
        )
    for i, ref in enumerate((coef_x, coef_y, coef_mix)):
        loads.append(
            pltpu.make_async_copy(ref, raw.at[i, pl.ds(PAD, ROWS)], load_sem.at[own + i])
        )
    for load in loads:
        load.start()

    x, z, y = me // 8, (me // 4) % 2, me % 4
    x_size = parts // 8
    x_near = [lax.rem(x + i, x_size) * 8 + z * 4 + y for i in (1, x_size - 1)]
    z_near = [x * 8 + (1 - z) * 4 + y]
    y_near = [x * 8 + z * 4 + lax.rem(y + i, 4) for i in (1, 3)]
    if x_size == 1:
        x_near = []

    def signal(semaphore, peers):
        for one in peers:
            pl.semaphore_signal(
                semaphore, inc=1, device_id=(one, tile), device_id_type=MESH
            )

    barrier = pltpu.get_barrier_semaphore()
    pl.semaphore_signal(barrier, inc=1, device_id=(me, below), device_id_type=MESH)
    pl.semaphore_signal(barrier, inc=1, device_id=(me, above), device_id_type=MESH)
    signal(barrier, y_near + z_near + x_near)
    pl.semaphore_wait(barrier, 2 + len(y_near + z_near + x_near))

    def spread_news():
        for number, peers in enumerate((y_near, x_near, x_near, z_near)):
            if peers:
                signal(news_sem.at[number], peers)
                yield
                pl.semaphore_wait(news_sem.at[number], len(peers))

    for load in loads:
        load.wait()

    halo = []
    for number, (target, src, dst) in enumerate(
        (
            (below, PAD + ROWS - PASSES, PAD - PASSES),
            (above, PAD, PAD + ROWS),
        )
    ):
        halo.append(
            pltpu.make_async_remote_copy(
                src_ref=levels.at[0, pl.ds(src, PASSES)],
                dst_ref=levels.at[0, pl.ds(dst, PASSES)],
                send_sem=halo_send.at[number],
                recv_sem=halo_recv.at[number],
                device_id=(me, target),
                device_id_type=MESH,
            )
        )
    for number, (target, src, dst) in enumerate(
        ((below, ROWS, 0), (above, PAD, PAD + ROWS))
    ):
        halo.append(
            pltpu.make_async_remote_copy(
                src_ref=raw.at[:, pl.ds(src, PAD)],
                dst_ref=raw.at[:, pl.ds(dst, PAD)],
                send_sem=halo_send.at[2 + number],
                recv_sem=halo_recv.at[2 + number],
                device_id=(me, target),
                device_id_type=MESH,
            )
        )
    for copy in halo:
        copy.start()

    def widen(row, carry):
        sx = raw[0, pl.ds(row, 1), :]
        sy = raw[1, pl.ds(row, 1), :]
        mix = raw[2, pl.ds(row, 1), :]
        for i, value in enumerate((1.0 - sx - sy - 4.0 * mix, sx + mix, sy + mix, mix)):
            coef[i, row] = jnp.broadcast_to(value, (8, width))
        return carry

    def advance(level, row):
        for half in range(own // 8):
            at = pl.ds(8 * half, 8)
            middle = levels[level, row, at, :]
            north = levels[level, row - 1, at, :]
            south = levels[level, row + 1, at, :]
            west = pltpu.roll(middle, 1, 1)
            east = pltpu.roll(middle, width - 1, 1)
            levels[level + 1, row, at, :] = (
                coef[0, row] * middle + coef[1, row] * west
            ) + (coef[2, row] * north + coef[3, row] * (south + east))

    def step(level, first, count):
        def several(i, carry):
            for j in range(UNROLL):
                advance(level, first + UNROLL * i + j)
            return carry

        trips = count // UNROLL
        lax.fori_loop(0, trips, several, 0)
        for row in range(first + UNROLL * trips, first + count):
            advance(level, row)

    group = lax.broadcasted_iota(jnp.int32, (8, 128), 1) // COLS

    def pack(g, carry):
        lanes = pl.ds(pl.multiple_of(g * 128, 128), 128)
        for half in range(own // 8):
            at = pl.ds(8 * half, 8)
            for block in range(lane_tiles):
                rows = [
                    levels[PASSES, PAD + 8 * g + r, at, pl.ds(128 * block, 128)]
                    for r in range(8)
                ]
                for p, value in enumerate(exchange_groups(rows, group)):
                    packed[8 * block + p, at, lanes] = value
        return carry

    lax.fori_loop(PAD, PAD + ROWS, widen, 0, unroll=4)
    news = spread_news()
    for k in range(1, PASSES + 1):
        step(k - 1, PAD + k, ROWS - 2 * k)
        next(news, None)
    lax.fori_loop(1, ROWS // 8 - 1, pack, 0)
    for copy in halo:
        copy.wait_recv()
    lax.fori_loop(PAD - PASSES, PAD, widen, 0, unroll=6)
    lax.fori_loop(PAD + ROWS, PAD + ROWS + PASSES, widen, 0, unroll=6)
    for k in range(1, PASSES + 1):
        for i in range(PASSES):
            advance(k - 1, PAD - PASSES + k + i)
            advance(k - 1, PAD + ROWS - k + i)
    pack(0, 0)
    pack(ROWS // 8 - 1, 0)
    for _ in news:
        pass

    def pick(b, carry):
        index = jnp.broadcast_to(obs_index[0, pl.ds(b, 1), :], (8, nobs))
        lane = index % 128
        place = index // 128
        for half in range(own // 8):
            at = pl.ds(8 * half, 8)
            total = jnp.zeros((8, nobs), jnp.float32)
            for g in range(cells // 128):
                found = jnp.take_along_axis(
                    packed[b, at, pl.ds(128 * g, 128)], lane, axis=1, mode="promise_in_bounds"
                )
                total = jnp.where(place == g, found, total)
            picked[b + 1, at, :] = total
        return carry

    lax.fori_loop(0, parts, pick, 0, unroll=4)
    picked[0] = picked[parts]
    picked[parts + 1] = picked[1]

    mine = pl.ds(pl.multiple_of(own * me, own), own)

    def seen_copy(k):
        return pltpu.make_async_remote_copy(
            src_ref=picked.at[pl.ds(peer(k), 3)],
            dst_ref=seen.at[:, mine],
            send_sem=seen_send.at[k],
            recv_sem=seen_recv.at[me],
            device_id=(peer(k), tile),
            device_id_type=MESH,
        )

    piece = cells // CHUNKS

    def patch_copy(c):
        lanes = pl.ds(piece * c, piece)

        def one(k):
            return pltpu.make_async_remote_copy(
                src_ref=packed.at[peer(k), :, lanes],
                dst_ref=members.at[mine, lanes],
                send_sem=patch_send.at[c, k],
                recv_sem=patch_recv.at[c, me],
                device_id=(peer(k), tile),
                device_id_type=MESH,
            )

        return one

    def back_copy(c):
        lanes = pl.ds(piece * c, piece)

        def one(k):
            rows = pl.ds(pl.multiple_of(own * peer(k), own), own)
            return pltpu.make_async_remote_copy(
                src_ref=result.at[rows, lanes],
                dst_ref=back.at[me, :, lanes],
                send_sem=back_send.at[c, k],
                recv_sem=back_recv.at[c, me],
                device_id=(peer(k), tile),
                device_id_type=MESH,
            )

        return one

    def seen_arrival(k):
        rows = pl.ds(pl.multiple_of(own * source(k), own), own)
        return pltpu.make_async_remote_copy(
            src_ref=picked.at[pl.ds(0, 3)],
            dst_ref=seen.at[:, rows],
            send_sem=seen_send.at[k],
            recv_sem=seen_recv.at[source(k)],
            device_id=(peer(k), tile),
            device_id_type=MESH,
        )

    def patch_arrival(c):
        lanes = pl.ds(piece * c, piece)

        def one(k):
            rows = pl.ds(pl.multiple_of(own * source(k), own), own)
            return pltpu.make_async_remote_copy(
                src_ref=packed.at[0, :, lanes],
                dst_ref=members.at[rows, lanes],
                send_sem=patch_send.at[c, k],
                recv_sem=patch_recv.at[c, source(k)],
                device_id=(peer(k), tile),
                device_id_type=MESH,
            )

        return one

    def back_arrival(c):
        lanes = pl.ds(piece * c, piece)

        def one(k):
            return pltpu.make_async_remote_copy(
                src_ref=result.at[pl.ds(0, own), lanes],
                dst_ref=back.at[source(k), :, lanes],
                send_sem=back_send.at[c, k],
                recv_sem=back_recv.at[c, source(k)],
                device_id=(peer(k), tile),
                device_id_type=MESH,
            )

        return one

    def for_all(make, act):
        def one(k, carry):
            act(make(k))
            return carry

        lax.fori_loop(1, parts, one, 0)

    start = lambda copy: copy.start()
    wait_send = lambda copy: copy.wait_send()
    wait_recv = lambda copy: copy.wait_recv()

    for_all(seen_copy, start)
    for role in range(3):
        seen[role, mine, :] = picked[me + role]
    members[mine, :] = packed[me]
    for_all(seen_arrival, wait_recv)
    for c in range(CHUNKS):
        for_all(patch_copy(c), start)

    row_id = lax.broadcasted_iota(jnp.int32, (size, size), 0)
    column_id = lax.broadcasted_iota(jnp.int32, (size, size), 1)
    diagonal = row_id == column_id
    gram = jnp.where(diagonal, size - 1.0, 0.0)
    pull = jnp.zeros((size, 1), jnp.float32)
    for role in range(3):
        patch = lax.rem(me + role + parts - 1, parts)
        value = obs_value[0, pl.ds(patch, 1), :]
        error = obs_error[0, pl.ds(patch, 1), :]
        level = loc_index[0, pl.ds(patch, 1), :]
        weight = jnp.zeros_like(value)
        for i in range(loc_table.shape[1]):
            weight = weight + jnp.where(level == i, loc_table[role, i], 0.0)
        precision = weight / error
        observed = seen[role]
        obs_mean = jnp.sum(observed, axis=0, keepdims=True) * (1.0 / size)
        spread = observed - obs_mean
        pull = pull + jnp.sum(
            spread * (precision * (value - obs_mean)), axis=1, keepdims=True
        )
        left_high, left_low = split(spread * precision)
        right_high, right_low = split(spread)
        gram = gram + sum(
            lax.dot_general(
                a, b, (((1,), (1,)), ((), ())), preferred_element_type=jnp.float32
            )
            for a, b in (
                (left_high, right_high),
                (left_high, right_low),
                (left_low, right_high),
                (left_low, right_low),
            )
        )
    square = jnp.sum(jnp.sum(gram * gram, axis=0, keepdims=True), axis=1, keepdims=True)
    inverse_scale = 1.0 / jnp.sqrt(square)

    def put(parts_ref, value):
        high, low = split(value)
        parts_ref[0] = high
        parts_ref[1] = low

    def product(a, b):
        return dot3(a[0], a[1], b[0], b[1])

    scaled = gram * inverse_scale
    put(matrix_parts, scaled)
    factor = jnp.where(diagonal, 1.5, 0.0) - 0.5 * scaled
    put(factor_parts, factor)
    put(root_parts, factor)
    put(matrix_parts, product(matrix_parts, factor_parts))

    def iterate(i, carry):
        put(
            factor_parts,
            jnp.where(diagonal, 1.5, 0.0) - 0.5 * product(root_parts, matrix_parts),
        )
        put(matrix_parts, product(matrix_parts, factor_parts))
        put(root_parts, product(factor_parts, root_parts))
        return carry

    lax.fori_loop(0, NS_ITERS - 2, iterate, 0)
    put(
        factor_parts,
        jnp.where(diagonal, 1.5, 0.0) - 0.5 * product(root_parts, matrix_parts),
    )
    root[...] = product(factor_parts, root_parts)

    pull_row = jnp.sum(jnp.where(diagonal, pull, 0.0), axis=0, keepdims=True)
    once = jnp.sum(root[...] * pull_row, axis=1, keepdims=True)
    mean_weight = jnp.sum(root[...] * once, axis=0, keepdims=True) * inverse_scale
    put(root_parts, jnp.sqrt((size - 1.0) * inverse_scale) * root[...] + mean_weight)

    width_at_once = min(piece, 256)
    for c in range(CHUNKS):
        for_all(patch_arrival(c), wait_recv)
        for first in range(piece * c, piece * (c + 1), width_at_once):
            lanes = pl.ds(first, width_at_once)
            block = members[:, lanes]
            center = jnp.sum(block, axis=0, keepdims=True) * (1.0 / size)
            high, low = split(block - center)
            result[:, lanes] = center + dot3(root_parts[0], root_parts[1], high, low)
        for_all(back_copy(c), start)

    def unpack(g, carry):
        lanes = pl.ds(pl.multiple_of(g * 128, 128), 128)
        for half in range(own // 8):
            at = pl.ds(8 * half, 8)
            for block in range(lane_tiles):
                values = [back[8 * block + p, at, lanes] for p in range(8)]
                for r, value in enumerate(exchange_groups(values, group)):
                    levels[0, 8 * g + r, at, pl.ds(128 * block, 128)] = value
        return carry

    back[me] = result[mine, :]
    for copy in halo:
        copy.wait_send()
    stores = []
    for c in range(CHUNKS):
        for_all(back_arrival(c), wait_recv)
        groups = ROWS // 8 // CHUNKS
        lax.fori_loop(groups * c, groups * (c + 1), unpack, 0)
        rows = pl.ds(ROWS // CHUNKS * c, ROWS // CHUNKS)
        for m in range(own):
            store = pltpu.make_async_copy(
                levels.at[0, rows, m], out.at[m, rows], out_sem.at[c, m]
            )
            store.start()
            stores.append(store)
    for_all(seen_copy, wait_send)
    for c in range(CHUNKS):
        for_all(patch_copy(c), wait_send)
        for_all(back_copy(c), wait_send)
    for store in stores:
        store.wait()


def body(*args, parts, tiles):
    field = args[0]
    own, _, width = field.shape
    size = own * parts
    cells = ROWS * COLS
    nobs = args[4].shape[2]
    f32 = jnp.float32
    dma = pltpu.SemaphoreType.DMA
    hbm = pl.BlockSpec(memory_space=pl.ANY)
    vmem = pl.BlockSpec(memory_space=pltpu.VMEM)
    smem = pl.BlockSpec(memory_space=pltpu.SMEM)
    tall = ROWS + 2 * PAD
    pair = pltpu.VMEM((2, size, size), jnp.bfloat16)
    return pl.pallas_call(
        functools.partial(main_kernel, parts=parts, tiles=tiles),
        out_shape=jax.ShapeDtypeStruct(field.shape, f32),
        in_specs=[hbm] * 4 + [vmem] * 4 + [smem],
        out_specs=hbm,
        scratch_shapes=[
            pltpu.VMEM((PASSES + 1, tall, own, width), f32),
            pltpu.VMEM((3, tall, width), f32),
            pltpu.VMEM((4, tall, 8, width), f32),
            pltpu.VMEM((parts, own, cells), f32),
            pltpu.VMEM((parts + 2, own, nobs), f32),
            pltpu.VMEM((size, cells), f32),
            pltpu.VMEM((3, size, nobs), f32),
            pltpu.VMEM((size, size), f32),
            pair,
            pair,
            pair,
            pltpu.VMEM((parts, own, cells), f32),
            pltpu.VMEM((size, cells), f32),
            dma((own + 3,)),
            dma((CHUNKS, own)),
            pltpu.SemaphoreType.REGULAR((4,)),
            dma((4,)),
            dma((4,)),
            dma((parts,)),
            dma((parts,)),
            dma((CHUNKS, parts)),
            dma((CHUNKS, parts)),
            dma((CHUNKS, parts)),
            dma((CHUNKS, parts)),
        ],
        compiler_params=pltpu.CompilerParams(
            collective_id=0, has_side_effects=True, vmem_limit_bytes=VMEM_LIMIT
        ),
        name="forecast_and_analysis",
    )(*args)


def solution(mesh):
    parts, tiles = mesh.shape["mem"], mesh.shape["tile"]
    in_specs = (
        P("mem", "tile", None),
        P("tile", None),
        P("tile", None),
        P("tile", None),
        P("tile", None, None),
        P("tile", None, None),
        P("tile", None, None),
        P("tile", None, None),
        P(),
    )
    return jax.shard_map(
        functools.partial(body, parts=parts, tiles=tiles),
        mesh=mesh,
        in_specs=in_specs,
        out_specs=P("mem", "tile", None),
        check_vma=False,
    )
```

```python
import functools

import jax
import jax.numpy as jnp
from jax import lax
from jax.experimental import pallas as pl
from jax.experimental.pallas import tpu as pltpu
from jax.sharding import PartitionSpec as P

PASSES = 6
NS_ITERS = 8
PAD = 8
ROWS = 64
COLS = 16
UNROLL = 16
CHUNKS = 4
EARLY = 1
ORDER = (1, 2, 3, 4, 5, 6, 0, 7)
MESH = pl.DeviceIdType.MESH
VMEM_LIMIT = 62 * 1024 * 1024


def split(x):
    high = x.astype(jnp.bfloat16)
    low = (x - high.astype(jnp.float32)).astype(jnp.bfloat16)
    return high, low


def dot(a, b):
    return jnp.dot(a, b, preferred_element_type=jnp.float32)


def dot3(a_high, a_low, b_high, b_low):
    return dot(a_high, b_high) + (dot(a_high, b_low) + dot(a_low, b_high))


def exchange_groups(rows, group):
    rows = list(rows)
    for bit in range(3):
        step = 1 << bit
        keep = (group & step) == 0
        for i in range(8):
            if i & step:
                continue
            a, b = rows[i], rows[i + step]
            rows[i] = jnp.where(keep, a, pltpu.roll(b, COLS * step, 1))
            rows[i + step] = jnp.where(keep, pltpu.roll(a, 128 - COLS * step, 1), b)
    return rows


def main_kernel(
    field,
    coef_x,
    coef_y,
    coef_mix,
    obs_value,
    obs_error,
    obs_index,
    loc_index,
    loc_table,
    out,
    levels,
    raw,
    coef,
    packed,
    picked,
    members,
    seen,
    root,
    matrix_parts,
    root_parts,
    factor_parts,
    back,
    result,
    load_sem,
    out_sem,
    news_sem,
    halo_send,
    halo_recv,
    seen_send,
    seen_recv,
    patch_send,
    patch_recv,
    back_send,
    back_recv,
    *,
    parts,
    tiles,
):
    me = lax.axis_index("mem")
    tile = lax.axis_index("tile")
    own = field.shape[0]
    width = field.shape[2]
    size = own * parts
    cells = ROWS * COLS
    nobs = obs_value.shape[2]
    lane_tiles = width // 128
    below = lax.rem(tile + 1, tiles)
    above = lax.rem(tile + tiles - 1, tiles)

    def peer(k):
        return lax.rem(me + 11 * k, parts)

    def source(k):
        return lax.rem(me + 12 * parts - 11 * k, parts)

    loads = []
    for m in range(own):
        loads.append(
            pltpu.make_async_copy(
                field.at[m], levels.at[0, pl.ds(PAD, ROWS), m], load_sem.at[m]
            )
        )
    for i, ref in enumerate((coef_x, coef_y, coef_mix)):
        loads.append(
            pltpu.make_async_copy(ref, raw.at[i, pl.ds(PAD, ROWS)], load_sem.at[own + i])
        )
    for load in loads:
        load.start()

    x, z, y = me // 8, (me // 4) % 2, me % 4
    x_size = parts // 8
    x_near = [lax.rem(x + i, x_size) * 8 + z * 4 + y for i in (1, x_size - 1)]
    z_near = [x * 8 + (1 - z) * 4 + y]
    y_near = [x * 8 + z * 4 + lax.rem(y + i, 4) for i in (1, 3)]
    if x_size == 1:
        x_near = []

    def signal(semaphore, peers):
        for one in peers:
            pl.semaphore_signal(
                semaphore, inc=1, device_id=(one, tile), device_id_type=MESH
            )

    barrier = pltpu.get_barrier_semaphore()
    pl.semaphore_signal(barrier, inc=1, device_id=(me, below), device_id_type=MESH)
    pl.semaphore_signal(barrier, inc=1, device_id=(me, above), device_id_type=MESH)
    signal(barrier, y_near + z_near + x_near)
    pl.semaphore_wait(barrier, 2 + len(y_near + z_near + x_near))

    def spread_news():
        for number, peers in enumerate((y_near, x_near, x_near, z_near)):
            if peers:
                signal(news_sem.at[number], peers)
                yield
                pl.semaphore_wait(news_sem.at[number], len(peers))

    for load in loads:
        load.wait()

    halo = []
    for number, (target, src, dst) in enumerate(
        (
            (below, PAD + ROWS - PASSES, PAD - PASSES),
            (above, PAD, PAD + ROWS),
        )
    ):
        halo.append(
            pltpu.make_async_remote_copy(
                src_ref=levels.at[0, pl.ds(src, PASSES)],
                dst_ref=levels.at[0, pl.ds(dst, PASSES)],
                send_sem=halo_send.at[number],
                recv_sem=halo_recv.at[number],
                device_id=(me, target),
                device_id_type=MESH,
            )
        )
    for number, (target, src, dst) in enumerate(
        ((below, ROWS, 0), (above, PAD, PAD + ROWS))
    ):
        halo.append(
            pltpu.make_async_remote_copy(
                src_ref=raw.at[:, pl.ds(src, PAD)],
                dst_ref=raw.at[:, pl.ds(dst, PAD)],
                send_sem=halo_send.at[2 + number],
                recv_sem=halo_recv.at[2 + number],
                device_id=(me, target),
                device_id_type=MESH,
            )
        )
    for copy in halo:
        copy.start()

    def widen(row, carry):
        sx = raw[0, pl.ds(row, 1), :]
        sy = raw[1, pl.ds(row, 1), :]
        mix = raw[2, pl.ds(row, 1), :]
        for i, value in enumerate((1.0 - sx - sy - 4.0 * mix, sx + mix, sy + mix, mix)):
            coef[i, row] = jnp.broadcast_to(value, (8, width))
        return carry

    def advance(level, row):
        for half in range(own // 8):
            at = pl.ds(8 * half, 8)
            middle = levels[level, row, at, :]
            north = levels[level, row - 1, at, :]
            south = levels[level, row + 1, at, :]
            west = pltpu.roll(middle, 1, 1)
            east = pltpu.roll(middle, width - 1, 1)
            levels[level + 1, row, at, :] = (
                coef[0, row] * middle + coef[1, row] * west
            ) + (coef[2, row] * north + coef[3, row] * (south + east))

    def step(level, first, count):
        def several(i, carry):
            for j in range(UNROLL):
                advance(level, first + UNROLL * i + j)
            return carry

        trips = count // UNROLL
        lax.fori_loop(0, trips, several, 0)
        for row in range(first + UNROLL * trips, first + count):
            advance(level, row)

    group = lax.broadcasted_iota(jnp.int32, (8, 128), 1) // COLS

    def pack(place, g):
        lanes = pl.ds(pl.multiple_of(place * 128, 128), 128)
        for half in range(own // 8):
            at = pl.ds(8 * half, 8)
            for block in range(lane_tiles):
                rows = [
                    levels[PASSES, PAD + 8 * g + r, at, pl.ds(128 * block, 128)]
                    for r in range(8)
                ]
                for p, value in enumerate(exchange_groups(rows, group)):
                    packed[8 * block + p, at, lanes] = value

    def pack_inner(place, carry):
        pack(place, place + 1)
        return carry

    mine = pl.ds(pl.multiple_of(own * me, own), own)

    def seen_copy(k):
        return pltpu.make_async_remote_copy(
            src_ref=picked.at[pl.ds(peer(k), 3)],
            dst_ref=seen.at[:, mine],
            send_sem=seen_send.at[k],
            recv_sem=seen_recv.at[me],
            device_id=(peer(k), tile),
            device_id_type=MESH,
        )

    piece = cells // CHUNKS

    def patch_copy(c):
        lanes = pl.ds(piece * c, piece)

        def one(k):
            return pltpu.make_async_remote_copy(
                src_ref=packed.at[peer(k), :, lanes],
                dst_ref=members.at[mine, lanes],
                send_sem=patch_send.at[c, k],
                recv_sem=patch_recv.at[c, me],
                device_id=(peer(k), tile),
                device_id_type=MESH,
            )

        return one

    def back_copy(c):
        lanes = pl.ds(piece * c, piece)

        def one(k):
            rows = pl.ds(pl.multiple_of(own * peer(k), own), own)
            return pltpu.make_async_remote_copy(
                src_ref=result.at[rows, lanes],
                dst_ref=back.at[me, :, lanes],
                send_sem=back_send.at[c, k],
                recv_sem=back_recv.at[c, me],
                device_id=(peer(k), tile),
                device_id_type=MESH,
            )

        return one

    def seen_arrival(k):
        rows = pl.ds(pl.multiple_of(own * source(k), own), own)
        return pltpu.make_async_remote_copy(
            src_ref=picked.at[pl.ds(0, 3)],
            dst_ref=seen.at[:, rows],
            send_sem=seen_send.at[k],
            recv_sem=seen_recv.at[source(k)],
            device_id=(peer(k), tile),
            device_id_type=MESH,
        )

    def patch_arrival(c):
        lanes = pl.ds(piece * c, piece)

        def one(k):
            rows = pl.ds(pl.multiple_of(own * source(k), own), own)
            return pltpu.make_async_remote_copy(
                src_ref=packed.at[0, :, lanes],
                dst_ref=members.at[rows, lanes],
                send_sem=patch_send.at[c, k],
                recv_sem=patch_recv.at[c, source(k)],
                device_id=(peer(k), tile),
                device_id_type=MESH,
            )

        return one

    def back_arrival(c):
        lanes = pl.ds(piece * c, piece)

        def one(k):
            return pltpu.make_async_remote_copy(
                src_ref=result.at[pl.ds(0, own), lanes],
                dst_ref=back.at[source(k), :, lanes],
                send_sem=back_send.at[c, k],
                recv_sem=back_recv.at[c, source(k)],
                device_id=(peer(k), tile),
                device_id_type=MESH,
            )

        return one

    def for_all(make, act):
        def one(k, carry):
            act(make(k))
            return carry

        lax.fori_loop(1, parts, one, 0)

    start = lambda copy: copy.start()
    wait_send = lambda copy: copy.wait_send()
    wait_recv = lambda copy: copy.wait_recv()

    lax.fori_loop(PAD, PAD + ROWS, widen, 0, unroll=4)
    news = spread_news()
    for k in range(1, PASSES + 1):
        step(k - 1, PAD + k, ROWS - 2 * k)
        next(news, None)
    for _ in news:
        pass
    per_chunk = ROWS // 8 // CHUNKS
    inner = ROWS // 8 - 2
    lax.fori_loop(0, per_chunk * EARLY, pack_inner, 0)
    for c in range(EARLY):
        for_all(patch_copy(c), start)
    lax.fori_loop(per_chunk * EARLY, inner, pack_inner, 0)
    for copy in halo:
        copy.wait_recv()
    lax.fori_loop(PAD - PASSES, PAD, widen, 0, unroll=6)
    lax.fori_loop(PAD + ROWS, PAD + ROWS + PASSES, widen, 0, unroll=6)
    for k in range(1, PASSES + 1):
        for i in range(PASSES):
            advance(k - 1, PAD - PASSES + k + i)
            advance(k - 1, PAD + ROWS - k + i)
    for place in range(inner, ROWS // 8):
        pack(place, ORDER[place])

    def pick(b, carry):
        index = jnp.broadcast_to(obs_index[0, pl.ds(b, 1), :], (8, nobs))
        lane = index % 128
        place = index // 128
        for half in range(own // 8):
            at = pl.ds(8 * half, 8)
            total = jnp.zeros((8, nobs), jnp.float32)
            for g in range(cells // 128):
                found = jnp.take_along_axis(
                    packed[b, at, pl.ds(128 * g, 128)], lane, axis=1, mode="promise_in_bounds"
                )
                total = jnp.where(place == ORDER[g], found, total)
            picked[b + 1, at, :] = total
        return carry

    lax.fori_loop(0, parts, pick, 0, unroll=4)
    picked[0] = picked[parts]
    picked[parts + 1] = picked[1]

    for_all(seen_copy, start)
    for role in range(3):
        seen[role, mine, :] = picked[me + role]
    members[mine, :] = packed[me]
    for_all(seen_arrival, wait_recv)
    for c in range(EARLY, CHUNKS):
        for_all(patch_copy(c), start)

    row_id = lax.broadcasted_iota(jnp.int32, (size, size), 0)
    column_id = lax.broadcasted_iota(jnp.int32, (size, size), 1)
    diagonal = row_id == column_id
    gram = jnp.where(diagonal, size - 1.0, 0.0)
    pull = jnp.zeros((size, 1), jnp.float32)
    for role in range(3):
        patch = lax.rem(me + role + parts - 1, parts)
        value = obs_value[0, pl.ds(patch, 1), :]
        error = obs_error[0, pl.ds(patch, 1), :]
        level = loc_index[0, pl.ds(patch, 1), :]
        weight = jnp.zeros_like(value)
        for i in range(loc_table.shape[1]):
            weight = weight + jnp.where(level == i, loc_table[role, i], 0.0)
        precision = weight / error
        observed = seen[role]
        obs_mean = jnp.sum(observed, axis=0, keepdims=True) * (1.0 / size)
        spread = observed - obs_mean
        pull = pull + jnp.sum(
            spread * (precision * (value - obs_mean)), axis=1, keepdims=True
        )
        left_high, left_low = split(spread * precision)
        right_high, right_low = split(spread)
        gram = gram + sum(
            lax.dot_general(
                a, b, (((1,), (1,)), ((), ())), preferred_element_type=jnp.float32
            )
            for a, b in (
                (left_high, right_high),
                (left_high, right_low),
                (left_low, right_high),
                (left_low, right_low),
            )
        )
    square = jnp.sum(jnp.sum(gram * gram, axis=0, keepdims=True), axis=1, keepdims=True)
    inverse_scale = 1.0 / jnp.sqrt(square)

    def put(parts_ref, value):
        high, low = split(value)
        parts_ref[0] = high
        parts_ref[1] = low

    def product(a, b):
        return dot3(a[0], a[1], b[0], b[1])

    scaled = gram * inverse_scale
    put(matrix_parts, scaled)
    factor = jnp.where(diagonal, 1.5, 0.0) - 0.5 * scaled
    put(factor_parts, factor)
    put(root_parts, factor)
    put(matrix_parts, product(matrix_parts, factor_parts))

    def iterate(i, carry):
        put(
            factor_parts,
            jnp.where(diagonal, 1.5, 0.0) - 0.5 * product(root_parts, matrix_parts),
        )
        put(matrix_parts, product(matrix_parts, factor_parts))
        put(root_parts, product(factor_parts, root_parts))
        return carry

    lax.fori_loop(0, NS_ITERS - 2, iterate, 0)
    put(
        factor_parts,
        jnp.where(diagonal, 1.5, 0.0) - 0.5 * product(root_parts, matrix_parts),
    )
    root[...] = product(factor_parts, root_parts)

    pull_row = jnp.sum(jnp.where(diagonal, pull, 0.0), axis=0, keepdims=True)
    once = jnp.sum(root[...] * pull_row, axis=1, keepdims=True)
    mean_weight = jnp.sum(root[...] * once, axis=0, keepdims=True) * inverse_scale
    put(root_parts, jnp.sqrt((size - 1.0) * inverse_scale) * root[...] + mean_weight)

    width_at_once = min(piece, 256)
    for c in range(CHUNKS):
        for_all(patch_arrival(c), wait_recv)
        for first in range(piece * c, piece * (c + 1), width_at_once):
            lanes = pl.ds(first, width_at_once)
            block = members[:, lanes]
            center = jnp.sum(block, axis=0, keepdims=True) * (1.0 / size)
            high, low = split(block - center)
            result[:, lanes] = center + dot3(root_parts[0], root_parts[1], high, low)
        for_all(back_copy(c), start)

    def unpack(place, g):
        lanes = pl.ds(128 * place, 128)
        for half in range(own // 8):
            at = pl.ds(8 * half, 8)
            for block in range(lane_tiles):
                values = [back[8 * block + p, at, lanes] for p in range(8)]
                for r, value in enumerate(exchange_groups(values, group)):
                    levels[0, 8 * g + r, at, pl.ds(128 * block, 128)] = value

    back[me] = result[mine, :]
    for copy in halo:
        copy.wait_send()
    stores = []
    for c in range(CHUNKS):
        for_all(back_arrival(c), wait_recv)
        for place in range(per_chunk * c, per_chunk * (c + 1)):
            g = ORDER[place]
            unpack(place, g)
            rows = pl.ds(8 * g, 8)
            for m in range(own):
                store = pltpu.make_async_copy(
                    levels.at[0, rows, m], out.at[m, rows], out_sem.at[g, m]
                )
                store.start()
                stores.append(store)
    for_all(seen_copy, wait_send)
    for c in range(CHUNKS):
        for_all(patch_copy(c), wait_send)
        for_all(back_copy(c), wait_send)
    for store in stores:
        store.wait()


def body(*args, parts, tiles):
    field = args[0]
    own, _, width = field.shape
    size = own * parts
    cells = ROWS * COLS
    nobs = args[4].shape[2]
    f32 = jnp.float32
    dma = pltpu.SemaphoreType.DMA
    hbm = pl.BlockSpec(memory_space=pl.ANY)
    vmem = pl.BlockSpec(memory_space=pltpu.VMEM)
    smem = pl.BlockSpec(memory_space=pltpu.SMEM)
    tall = ROWS + 2 * PAD
    pair = pltpu.VMEM((2, size, size), jnp.bfloat16)
    return pl.pallas_call(
        functools.partial(main_kernel, parts=parts, tiles=tiles),
        out_shape=jax.ShapeDtypeStruct(field.shape, f32),
        in_specs=[hbm] * 4 + [vmem] * 4 + [smem],
        out_specs=hbm,
        scratch_shapes=[
            pltpu.VMEM((PASSES + 1, tall, own, width), f32),
            pltpu.VMEM((3, tall, width), f32),
            pltpu.VMEM((4, tall, 8, width), f32),
            pltpu.VMEM((parts, own, cells), f32),
            pltpu.VMEM((parts + 2, own, nobs), f32),
            pltpu.VMEM((size, cells), f32),
            pltpu.VMEM((3, size, nobs), f32),
            pltpu.VMEM((size, size), f32),
            pair,
            pair,
            pair,
            pltpu.VMEM((parts, own, cells), f32),
            pltpu.VMEM((size, cells), f32),
            dma((own + 3,)),
            dma((ROWS // 8, own)),
            pltpu.SemaphoreType.REGULAR((4,)),
            dma((4,)),
            dma((4,)),
            dma((parts,)),
            dma((parts,)),
            dma((CHUNKS, parts)),
            dma((CHUNKS, parts)),
            dma((CHUNKS, parts)),
            dma((CHUNKS, parts)),
        ],
        compiler_params=pltpu.CompilerParams(
            collective_id=0, has_side_effects=True, vmem_limit_bytes=VMEM_LIMIT
        ),
        name="forecast_and_analysis",
    )(*args)


def solution(mesh):
    parts, tiles = mesh.shape["mem"], mesh.shape["tile"]
    in_specs = (
        P("mem", "tile", None),
        P("tile", None),
        P("tile", None),
        P("tile", None),
        P("tile", None, None),
        P("tile", None, None),
        P("tile", None, None),
        P("tile", None, None),
        P(),
    )
    return jax.shard_map(
        functools.partial(body, parts=parts, tiles=tiles),
        mesh=mesh,
        in_specs=in_specs,
        out_specs=P("mem", "tile", None),
        check_vma=False,
    )
```

```python
import functools

import jax
import jax.numpy as jnp
from jax import lax
from jax.experimental import pallas as pl
from jax.experimental.pallas import tpu as pltpu
from jax.sharding import PartitionSpec as P

PASSES = 6
NS_ITERS = 8
PAD = 8
ROWS = 64
COLS = 16
UNROLL = 16
PIECES = ((0, 2), (2, 5), (5, 8))
EARLY = 1
ORDER = (1, 2, 3, 4, 5, 6, 0, 7)
MESH = pl.DeviceIdType.MESH
VMEM_LIMIT = 62 * 1024 * 1024


def split(x):
    high = x.astype(jnp.bfloat16)
    low = (x - high.astype(jnp.float32)).astype(jnp.bfloat16)
    return high, low


def dot(a, b):
    return jnp.dot(a, b, preferred_element_type=jnp.float32)


def dot3(a_high, a_low, b_high, b_low):
    return dot(a_high, b_high) + (dot(a_high, b_low) + dot(a_low, b_high))


def exchange_groups(rows, group):
    rows = list(rows)
    for bit in range(3):
        step = 1 << bit
        keep = (group & step) == 0
        for i in range(8):
            if i & step:
                continue
            a, b = rows[i], rows[i + step]
            rows[i] = jnp.where(keep, a, pltpu.roll(b, COLS * step, 1))
            rows[i + step] = jnp.where(keep, pltpu.roll(a, 128 - COLS * step, 1), b)
    return rows


def main_kernel(
    field,
    coef_x,
    coef_y,
    coef_mix,
    obs_value,
    obs_error,
    obs_index,
    loc_index,
    loc_table,
    out,
    levels,
    raw,
    coef,
    packed,
    picked,
    members,
    seen,
    root,
    matrix_parts,
    root_parts,
    factor_parts,
    back,
    result,
    load_sem,
    out_sem,
    news_sem,
    halo_send,
    halo_recv,
    seen_send,
    seen_recv,
    patch_send,
    patch_recv,
    back_send,
    back_recv,
    *,
    parts,
    tiles,
):
    me = lax.axis_index("mem")
    tile = lax.axis_index("tile")
    own = field.shape[0]
    width = field.shape[2]
    size = own * parts
    cells = ROWS * COLS
    nobs = obs_value.shape[2]
    lane_tiles = width // 128
    below = lax.rem(tile + 1, tiles)
    above = lax.rem(tile + tiles - 1, tiles)

    def peer(k):
        return lax.rem(me + 11 * k, parts)

    loads = []
    for m in range(own):
        loads.append(
            pltpu.make_async_copy(
                field.at[m], levels.at[0, pl.ds(PAD, ROWS), m], load_sem.at[m]
            )
        )
    for i, ref in enumerate((coef_x, coef_y, coef_mix)):
        loads.append(
            pltpu.make_async_copy(ref, raw.at[i, pl.ds(PAD, ROWS)], load_sem.at[own + i])
        )
    for load in loads:
        load.start()

    x, z, y = me // 8, (me // 4) % 2, me % 4
    x_size = parts // 8
    x_near = [lax.rem(x + i, x_size) * 8 + z * 4 + y for i in (1, x_size - 1)]
    z_near = [x * 8 + (1 - z) * 4 + y]
    y_near = [x * 8 + z * 4 + lax.rem(y + i, 4) for i in (1, 3)]
    if x_size == 1:
        x_near = []

    def signal(semaphore, peers):
        for one in peers:
            pl.semaphore_signal(
                semaphore, inc=1, device_id=(one, tile), device_id_type=MESH
            )

    barrier = pltpu.get_barrier_semaphore()
    pl.semaphore_signal(barrier, inc=1, device_id=(me, below), device_id_type=MESH)
    pl.semaphore_signal(barrier, inc=1, device_id=(me, above), device_id_type=MESH)
    signal(barrier, y_near + z_near + x_near)
    pl.semaphore_wait(barrier, 2 + len(y_near + z_near + x_near))

    def spread_news():
        for number, peers in enumerate((y_near, x_near, x_near, z_near)):
            if peers:
                signal(news_sem.at[number], peers)
                yield
                pl.semaphore_wait(news_sem.at[number], len(peers))

    for load in loads:
        load.wait()

    halo = []
    for number, (target, src, dst) in enumerate(
        (
            (below, PAD + ROWS - PASSES, PAD - PASSES),
            (above, PAD, PAD + ROWS),
        )
    ):
        halo.append(
            pltpu.make_async_remote_copy(
                src_ref=levels.at[0, pl.ds(src, PASSES)],
                dst_ref=levels.at[0, pl.ds(dst, PASSES)],
                send_sem=halo_send.at[number],
                recv_sem=halo_recv.at[number],
                device_id=(me, target),
                device_id_type=MESH,
            )
        )
    for number, (target, src, dst) in enumerate(
        ((below, ROWS, 0), (above, PAD, PAD + ROWS))
    ):
        halo.append(
            pltpu.make_async_remote_copy(
                src_ref=raw.at[:, pl.ds(src, PAD)],
                dst_ref=raw.at[:, pl.ds(dst, PAD)],
                send_sem=halo_send.at[2 + number],
                recv_sem=halo_recv.at[2 + number],
                device_id=(me, target),
                device_id_type=MESH,
            )
        )
    for copy in halo:
        copy.start()

    def widen(row, carry):
        sx = raw[0, pl.ds(row, 1), :]
        sy = raw[1, pl.ds(row, 1), :]
        mix = raw[2, pl.ds(row, 1), :]
        for i, value in enumerate((1.0 - sx - sy - 4.0 * mix, sx + mix, sy + mix, mix)):
            coef[i, row] = jnp.broadcast_to(value, (8, width))
        return carry

    def advance(level, row):
        for half in range(own // 8):
            at = pl.ds(8 * half, 8)
            middle = levels[level, row, at, :]
            north = levels[level, row - 1, at, :]
            south = levels[level, row + 1, at, :]
            west = pltpu.roll(middle, 1, 1)
            east = pltpu.roll(middle, width - 1, 1)
            levels[level + 1, row, at, :] = (
                coef[0, row] * middle + coef[1, row] * west
            ) + (coef[2, row] * north + coef[3, row] * (south + east))

    def step(level, first, count):
        def several(i, carry):
            for j in range(UNROLL):
                advance(level, first + UNROLL * i + j)
            return carry

        trips = count // UNROLL
        lax.fori_loop(0, trips, several, 0)
        for row in range(first + UNROLL * trips, first + count):
            advance(level, row)

    group = lax.broadcasted_iota(jnp.int32, (8, 128), 1) // COLS

    def pack(place, g):
        lanes = pl.ds(pl.multiple_of(place * 128, 128), 128)
        for half in range(own // 8):
            at = pl.ds(8 * half, 8)
            for block in range(lane_tiles):
                rows = [
                    levels[PASSES, PAD + 8 * g + r, at, pl.ds(128 * block, 128)]
                    for r in range(8)
                ]
                for p, value in enumerate(exchange_groups(rows, group)):
                    packed[8 * block + p, at, lanes] = value

    def pack_inner(place, carry):
        pack(place, place + 1)
        return carry

    mine = pl.ds(pl.multiple_of(own * me, own), own)

    def seen_copy(k):
        return pltpu.make_async_remote_copy(
            src_ref=picked.at[pl.ds(peer(k), 3)],
            dst_ref=seen.at[:, mine],
            send_sem=seen_send,
            recv_sem=seen_recv,
            device_id=(peer(k), tile),
            device_id_type=MESH,
        )

    others = parts - 1

    def lanes_of(c):
        first, last = PIECES[c]
        return pl.ds(128 * first, 128 * (last - first))

    def patch_copy(c):
        def one(k):
            return pltpu.make_async_remote_copy(
                src_ref=packed.at[peer(k), :, lanes_of(c)],
                dst_ref=members.at[mine, lanes_of(c)],
                send_sem=patch_send,
                recv_sem=patch_recv.at[c],
                device_id=(peer(k), tile),
                device_id_type=MESH,
            )

        return one

    def back_copy(c):
        def one(k):
            rows = pl.ds(pl.multiple_of(own * peer(k), own), own)
            return pltpu.make_async_remote_copy(
                src_ref=result.at[rows, lanes_of(c)],
                dst_ref=back.at[me, :, lanes_of(c)],
                send_sem=back_send,
                recv_sem=back_recv.at[c],
                device_id=(peer(k), tile),
                device_id_type=MESH,
            )

        return one

    def start_all(make):
        def one(k, carry):
            make(k).start()
            return carry

        lax.fori_loop(1, parts, one, 0)

    def together(src, dst, send_sem, recv_sem):
        return pltpu.make_async_remote_copy(
            src_ref=src,
            dst_ref=dst,
            send_sem=send_sem,
            recv_sem=recv_sem,
            device_id=(peer(1), tile),
            device_id_type=MESH,
        )

    most = pl.ds(0, own * others)
    seen_all = together(
        seen.at[:, most], seen.at[:, most], seen_send, seen_recv
    )

    def patch_all(c):
        return together(
            result.at[most, lanes_of(c)], members.at[most, lanes_of(c)], patch_send, patch_recv.at[c]
        )

    def back_all(c):
        src, dst = packed.at[pl.ds(0, others), :, lanes_of(c)], back.at[pl.ds(0, others), :, lanes_of(c)]
        return together(src, dst, back_send, back_recv.at[c])

    patch_sent = together(members.at[most], result.at[most], patch_send, patch_recv.at[0])
    back_sent = together(members.at[most], result.at[most], back_send, back_recv.at[0])

    lax.fori_loop(PAD, PAD + ROWS, widen, 0, unroll=4)
    news = spread_news()
    for k in range(1, PASSES + 1):
        step(k - 1, PAD + k, ROWS - 2 * k)
        next(news, None)
    for _ in news:
        pass
    inner = ROWS // 8 - 2
    packed_early = PIECES[EARLY][0]
    if packed_early:
        lax.fori_loop(0, packed_early, pack_inner, 0)
    for c in range(EARLY):
        start_all(patch_copy(c))
    lax.fori_loop(packed_early, inner, pack_inner, 0)
    for copy in halo:
        copy.wait_recv()
    lax.fori_loop(PAD - PASSES, PAD, widen, 0, unroll=6)
    lax.fori_loop(PAD + ROWS, PAD + ROWS + PASSES, widen, 0, unroll=6)
    for k in range(1, PASSES + 1):
        for i in range(PASSES):
            advance(k - 1, PAD - PASSES + k + i)
            advance(k - 1, PAD + ROWS - k + i)
    for place in range(inner, ROWS // 8):
        pack(place, ORDER[place])

    def pick(b, carry):
        index = jnp.broadcast_to(obs_index[0, pl.ds(b, 1), :], (8, nobs))
        lane = index % 128
        place = index // 128
        for half in range(own // 8):
            at = pl.ds(8 * half, 8)
            total = jnp.zeros((8, nobs), jnp.float32)
            for g in range(cells // 128):
                found = jnp.take_along_axis(
                    packed[b, at, pl.ds(128 * g, 128)], lane, axis=1, mode="promise_in_bounds"
                )
                total = jnp.where(place == ORDER[g], found, total)
            picked[b + 1, at, :] = total
        return carry

    lax.fori_loop(0, parts, pick, 0, unroll=4)
    picked[0] = picked[parts]
    picked[parts + 1] = picked[1]

    start_all(seen_copy)
    for role in range(3):
        seen[role, mine, :] = picked[me + role]
    members[mine, :] = packed[me]
    seen_all.wait_recv()
    for c in range(EARLY, len(PIECES)):
        start_all(patch_copy(c))

    row_id = lax.broadcasted_iota(jnp.int32, (size, size), 0)
    column_id = lax.broadcasted_iota(jnp.int32, (size, size), 1)
    diagonal = row_id == column_id
    gram = jnp.where(diagonal, size - 1.0, 0.0)
    pull = jnp.zeros((size, 1), jnp.float32)
    for role in range(3):
        patch = lax.rem(me + role + parts - 1, parts)
        value = obs_value[0, pl.ds(patch, 1), :]
        error = obs_error[0, pl.ds(patch, 1), :]
        level = loc_index[0, pl.ds(patch, 1), :]
        weight = jnp.zeros_like(value)
        for i in range(loc_table.shape[1]):
            weight = weight + jnp.where(level == i, loc_table[role, i], 0.0)
        precision = weight / error
        observed = seen[role]
        obs_mean = jnp.sum(observed, axis=0, keepdims=True) * (1.0 / size)
        spread = observed - obs_mean
        pull = pull + jnp.sum(
            spread * (precision * (value - obs_mean)), axis=1, keepdims=True
        )
        left_high, left_low = split(spread * precision)
        right_high, right_low = split(spread)
        gram = gram + sum(
            lax.dot_general(
                a, b, (((1,), (1,)), ((), ())), preferred_element_type=jnp.float32
            )
            for a, b in (
                (left_high, right_high),
                (left_high, right_low),
                (left_low, right_high),
                (left_low, right_low),
            )
        )
    square = jnp.sum(jnp.sum(gram * gram, axis=0, keepdims=True), axis=1, keepdims=True)
    inverse_scale = 1.0 / jnp.sqrt(square)

    def put(parts_ref, value):
        high, low = split(value)
        parts_ref[0] = high
        parts_ref[1] = low

    def product(a, b):
        return dot3(a[0], a[1], b[0], b[1])

    scaled = gram * inverse_scale
    put(matrix_parts, scaled)
    factor = jnp.where(diagonal, 1.5, 0.0) - 0.5 * scaled
    put(factor_parts, factor)
    put(root_parts, factor)
    put(matrix_parts, product(matrix_parts, factor_parts))

    def iterate(i, carry):
        put(
            factor_parts,
            jnp.where(diagonal, 1.5, 0.0) - 0.5 * product(root_parts, matrix_parts),
        )
        put(matrix_parts, product(matrix_parts, factor_parts))
        put(root_parts, product(factor_parts, root_parts))
        return carry

    lax.fori_loop(0, NS_ITERS - 2, iterate, 0)
    put(
        factor_parts,
        jnp.where(diagonal, 1.5, 0.0) - 0.5 * product(root_parts, matrix_parts),
    )
    root[...] = product(factor_parts, root_parts)

    pull_row = jnp.sum(jnp.where(diagonal, pull, 0.0), axis=0, keepdims=True)
    once = jnp.sum(root[...] * pull_row, axis=1, keepdims=True)
    mean_weight = jnp.sum(root[...] * once, axis=0, keepdims=True) * inverse_scale
    put(root_parts, jnp.sqrt((size - 1.0) * inverse_scale) * root[...] + mean_weight)

    for c, (first_block, last_block) in enumerate(PIECES):
        patch_all(c).wait_recv()
        for first in range(first_block, last_block, 2):
            many = min(2, last_block - first)
            lanes = pl.ds(128 * first, 128 * many)
            block = members[:, lanes]
            center = jnp.sum(block, axis=0, keepdims=True) * (1.0 / size)
            high, low = split(block - center)
            result[:, lanes] = center + dot3(root_parts[0], root_parts[1], high, low)
        start_all(back_copy(c))

    def unpack(place, g):
        lanes = pl.ds(128 * place, 128)
        for half in range(own // 8):
            at = pl.ds(8 * half, 8)
            for block in range(lane_tiles):
                values = [back[8 * block + p, at, lanes] for p in range(8)]
                for r, value in enumerate(exchange_groups(values, group)):
                    levels[0, 8 * g + r, at, pl.ds(128 * block, 128)] = value

    back[me] = result[mine, :]
    for copy in halo:
        copy.wait_send()
    stores = []
    for c, (first_block, last_block) in enumerate(PIECES):
        back_all(c).wait_recv()
        for place in range(first_block, last_block):
            g = ORDER[place]
            unpack(place, g)
            rows = pl.ds(8 * g, 8)
            for m in range(own):
                store = pltpu.make_async_copy(
                    levels.at[0, rows, m], out.at[m, rows], out_sem.at[g, m]
                )
                store.start()
                stores.append(store)
    seen_all.wait_send()
    patch_sent.wait_send()
    back_sent.wait_send()
    for store in stores:
        store.wait()


def body(*args, parts, tiles):
    field = args[0]
    own, _, width = field.shape
    size = own * parts
    cells = ROWS * COLS
    nobs = args[4].shape[2]
    f32 = jnp.float32
    dma = pltpu.SemaphoreType.DMA
    hbm = pl.BlockSpec(memory_space=pl.ANY)
    vmem = pl.BlockSpec(memory_space=pltpu.VMEM)
    smem = pl.BlockSpec(memory_space=pltpu.SMEM)
    tall = ROWS + 2 * PAD
    pair = pltpu.VMEM((2, size, size), jnp.bfloat16)
    return pl.pallas_call(
        functools.partial(main_kernel, parts=parts, tiles=tiles),
        out_shape=jax.ShapeDtypeStruct(field.shape, f32),
        in_specs=[hbm] * 4 + [vmem] * 4 + [smem],
        out_specs=hbm,
        scratch_shapes=[
            pltpu.VMEM((PASSES + 1, tall, own, width), f32),
            pltpu.VMEM((3, tall, width), f32),
            pltpu.VMEM((4, tall, 8, width), f32),
            pltpu.VMEM((parts, own, cells), f32),
            pltpu.VMEM((parts + 2, own, nobs), f32),
            pltpu.VMEM((size, cells), f32),
            pltpu.VMEM((3, size, nobs), f32),
            pltpu.VMEM((size, size), f32),
            pair,
            pair,
            pair,
            pltpu.VMEM((parts, own, cells), f32),
            pltpu.VMEM((size, cells), f32),
            dma((own + 3,)),
            dma((ROWS // 8, own)),
            pltpu.SemaphoreType.REGULAR((4,)),
            dma((4,)),
            dma((4,)),
            dma,
            dma,
            dma,
            dma((len(PIECES),)),
            dma,
            dma((len(PIECES),)),
        ],
        compiler_params=pltpu.CompilerParams(
            collective_id=0, has_side_effects=True, vmem_limit_bytes=VMEM_LIMIT
        ),
        name="forecast_and_analysis",
    )(*args)


def solution(mesh):
    parts, tiles = mesh.shape["mem"], mesh.shape["tile"]
    in_specs = (
        P("mem", "tile", None),
        P("tile", None),
        P("tile", None),
        P("tile", None),
        P("tile", None, None),
        P("tile", None, None),
        P("tile", None, None),
        P("tile", None, None),
        P(),
    )
    return jax.shard_map(
        functools.partial(body, parts=parts, tiles=tiles),
        mesh=mesh,
        in_specs=in_specs,
        out_specs=P("mem", "tile", None),
        check_vma=False,
    )
```

```python
import functools

import jax
import jax.numpy as jnp
from jax import lax
from jax.experimental import pallas as pl
from jax.experimental.pallas import tpu as pltpu
from jax.sharding import PartitionSpec as P

PASSES = 6
NS_ITERS = 8
PAD = 8
ROWS = 64
COLS = 16
UNROLL = 16
PIECES = ((0, 2), (2, 5), (5, 8))
EARLY = 1
ORDER = (1, 2, 3, 4, 5, 6, 0, 7)
MESH = pl.DeviceIdType.MESH
VMEM_LIMIT = 62 * 1024 * 1024


def split(x):
    high = x.astype(jnp.bfloat16)
    low = (x - high.astype(jnp.float32)).astype(jnp.bfloat16)
    return high, low


def dot(a, b):
    return jnp.dot(a, b, preferred_element_type=jnp.float32)


def dot3(a_high, a_low, b_high, b_low):
    return dot(a_high, b_high) + (dot(a_high, b_low) + dot(a_low, b_high))


def exchange_groups(rows, group):
    rows = list(rows)
    for bit in range(3):
        step = 1 << bit
        keep = (group & step) == 0
        for i in range(8):
            if i & step:
                continue
            a, b = rows[i], rows[i + step]
            rows[i] = jnp.where(keep, a, pltpu.roll(b, COLS * step, 1))
            rows[i + step] = jnp.where(keep, pltpu.roll(a, 128 - COLS * step, 1), b)
    return rows


def main_kernel(
    field,
    coef_x,
    coef_y,
    coef_mix,
    obs_value,
    obs_error,
    obs_index,
    loc_index,
    loc_table,
    out,
    levels,
    raw,
    coef,
    packed,
    picked,
    members,
    seen,
    root,
    matrix_parts,
    root_parts,
    factor_parts,
    back,
    result,
    load_sem,
    out_sem,
    news_sem,
    halo_send,
    halo_recv,
    seen_send,
    seen_recv,
    patch_send,
    patch_recv,
    back_send,
    back_recv,
    *,
    parts,
    tiles,
):
    me = lax.axis_index("mem")
    tile = lax.axis_index("tile")
    own = field.shape[0]
    width = field.shape[2]
    size = own * parts
    cells = ROWS * COLS
    nobs = obs_value.shape[2]
    lane_tiles = width // 128
    below = lax.rem(tile + 1, tiles)
    above = lax.rem(tile + tiles - 1, tiles)

    def peer(k):
        return lax.rem(me + 11 * k, parts)

    loads = []
    for m in range(own):
        loads.append(
            pltpu.make_async_copy(
                field.at[m], levels.at[0, pl.ds(PAD, ROWS), m], load_sem.at[m]
            )
        )
    for i, ref in enumerate((coef_x, coef_y, coef_mix)):
        loads.append(
            pltpu.make_async_copy(ref, raw.at[i, pl.ds(PAD, ROWS)], load_sem.at[own + i])
        )
    for load in loads:
        load.start()

    x, z, y = me // 8, (me // 4) % 2, me % 4
    x_size = parts // 8
    x_near = [lax.rem(x + i, x_size) * 8 + z * 4 + y for i in (1, x_size - 1)]
    z_near = [x * 8 + (1 - z) * 4 + y]
    y_near = [x * 8 + z * 4 + lax.rem(y + i, 4) for i in (1, 3)]
    if x_size == 1:
        x_near = []

    def signal(semaphore, peers):
        for one in peers:
            pl.semaphore_signal(
                semaphore, inc=1, device_id=(one, tile), device_id_type=MESH
            )

    barrier = pltpu.get_barrier_semaphore()
    pl.semaphore_signal(barrier, inc=1, device_id=(me, below), device_id_type=MESH)
    pl.semaphore_signal(barrier, inc=1, device_id=(me, above), device_id_type=MESH)
    signal(barrier, y_near + z_near + x_near)
    pl.semaphore_wait(barrier, 2 + len(y_near + z_near + x_near))

    def spread_news():
        for number, peers in enumerate((y_near, x_near, x_near, z_near)):
            if peers:
                signal(news_sem.at[number], peers)
                yield
                pl.semaphore_wait(news_sem.at[number], len(peers))

    for load in loads:
        load.wait()

    halo = []
    for number, (target, src, dst) in enumerate(
        (
            (below, PAD + ROWS - PASSES, PAD - PASSES),
            (above, PAD, PAD + ROWS),
        )
    ):
        halo.append(
            pltpu.make_async_remote_copy(
                src_ref=levels.at[0, pl.ds(src, PASSES)],
                dst_ref=levels.at[0, pl.ds(dst, PASSES)],
                send_sem=halo_send.at[number],
                recv_sem=halo_recv.at[number],
                device_id=(me, target),
                device_id_type=MESH,
            )
        )
    for number, (target, src, dst) in enumerate(
        ((below, ROWS, 0), (above, PAD, PAD + ROWS))
    ):
        halo.append(
            pltpu.make_async_remote_copy(
                src_ref=raw.at[:, pl.ds(src, PAD)],
                dst_ref=raw.at[:, pl.ds(dst, PAD)],
                send_sem=halo_send.at[2 + number],
                recv_sem=halo_recv.at[2 + number],
                device_id=(me, target),
                device_id_type=MESH,
            )
        )
    for copy in halo:
        copy.start()

    def widen(row, carry):
        sx = raw[0, pl.ds(row, 1), :]
        sy = raw[1, pl.ds(row, 1), :]
        mix = raw[2, pl.ds(row, 1), :]
        for i, value in enumerate((1.0 - sx - sy - 4.0 * mix, sx + mix, sy + mix, mix)):
            coef[i, row] = jnp.broadcast_to(value, (8, width))
        return carry

    def advance(level, row):
        for half in range(own // 8):
            at = pl.ds(8 * half, 8)
            middle = levels[level, row, at, :]
            north = levels[level, row - 1, at, :]
            south = levels[level, row + 1, at, :]
            west = pltpu.roll(middle, 1, 1)
            east = pltpu.roll(middle, width - 1, 1)
            levels[level + 1, row, at, :] = (
                coef[0, row] * middle + coef[1, row] * west
            ) + (coef[2, row] * north + coef[3, row] * (south + east))

    def step(level, first, count):
        def several(i, carry):
            for j in range(UNROLL):
                advance(level, first + UNROLL * i + j)
            return carry

        trips = count // UNROLL
        lax.fori_loop(0, trips, several, 0)
        for row in range(first + UNROLL * trips, first + count):
            advance(level, row)

    group = lax.broadcasted_iota(jnp.int32, (8, 128), 1) // COLS

    def pack(place, g):
        lanes = pl.ds(pl.multiple_of(place * 128, 128), 128)
        for half in range(own // 8):
            at = pl.ds(8 * half, 8)
            for block in range(lane_tiles):
                rows = [
                    levels[PASSES, PAD + 8 * g + r, at, pl.ds(128 * block, 128)]
                    for r in range(8)
                ]
                for p, value in enumerate(exchange_groups(rows, group)):
                    packed[8 * block + p, at, lanes] = value

    def pack_inner(place, carry):
        pack(place, place + 1)
        return carry

    mine = pl.ds(pl.multiple_of(own * me, own), own)

    def seen_copy(k):
        return pltpu.make_async_remote_copy(
            src_ref=picked.at[pl.ds(peer(k), 3)],
            dst_ref=seen.at[:, mine],
            send_sem=seen_send,
            recv_sem=seen_recv,
            device_id=(peer(k), tile),
            device_id_type=MESH,
        )

    others = parts - 1

    def lanes_of(c):
        first, last = PIECES[c]
        return pl.ds(128 * first, 128 * (last - first))

    def patch_copy(c):
        def one(k):
            return pltpu.make_async_remote_copy(
                src_ref=packed.at[peer(k), :, lanes_of(c)],
                dst_ref=members.at[mine, lanes_of(c)],
                send_sem=patch_send,
                recv_sem=patch_recv.at[c],
                device_id=(peer(k), tile),
                device_id_type=MESH,
            )

        return one

    def back_copy(c):
        def one(k):
            rows = pl.ds(pl.multiple_of(own * peer(k), own), own)
            return pltpu.make_async_remote_copy(
                src_ref=result.at[rows, lanes_of(c)],
                dst_ref=back.at[me, :, lanes_of(c)],
                send_sem=back_send,
                recv_sem=back_recv.at[c],
                device_id=(peer(k), tile),
                device_id_type=MESH,
            )

        return one

    def start_all(make):
        def one(k, carry):
            make(k).start()
            return carry

        lax.fori_loop(1, parts, one, 0)

    def together(src, dst, send_sem, recv_sem):
        return pltpu.make_async_remote_copy(
            src_ref=src,
            dst_ref=dst,
            send_sem=send_sem,
            recv_sem=recv_sem,
            device_id=(peer(1), tile),
            device_id_type=MESH,
        )

    most = pl.ds(0, own * others)
    seen_all = together(
        seen.at[:, most], seen.at[:, most], seen_send, seen_recv
    )

    def patch_all(c):
        return together(
            result.at[most, lanes_of(c)], members.at[most, lanes_of(c)], patch_send, patch_recv.at[c]
        )

    def back_all(c):
        src, dst = packed.at[pl.ds(0, others), :, lanes_of(c)], back.at[pl.ds(0, others), :, lanes_of(c)]
        return together(src, dst, back_send, back_recv.at[c])

    patch_sent = together(members.at[most], result.at[most], patch_send, patch_recv.at[0])
    back_sent = together(members.at[most], result.at[most], back_send, back_recv.at[0])

    lax.fori_loop(PAD, PAD + ROWS, widen, 0, unroll=4)
    news = spread_news()
    for k in range(1, PASSES + 1):
        step(k - 1, PAD + k, ROWS - 2 * k)
        next(news, None)
    for _ in news:
        pass
    inner = ROWS // 8 - 2
    packed_early = PIECES[EARLY][0]
    if packed_early:
        lax.fori_loop(0, packed_early, pack_inner, 0, unroll=2)
    for c in range(EARLY):
        start_all(patch_copy(c))
    lax.fori_loop(packed_early, inner, pack_inner, 0, unroll=2)
    for copy in halo:
        copy.wait_recv()
    lax.fori_loop(PAD - PASSES, PAD, widen, 0, unroll=6)
    lax.fori_loop(PAD + ROWS, PAD + ROWS + PASSES, widen, 0, unroll=6)
    for k in range(1, PASSES + 1):
        for i in range(PASSES):
            advance(k - 1, PAD - PASSES + k + i)
            advance(k - 1, PAD + ROWS - k + i)
    for place in range(inner, ROWS // 8):
        pack(place, ORDER[place])

    def pick(b, carry):
        index = jnp.broadcast_to(obs_index[0, pl.ds(b, 1), :], (8, nobs))
        lane = index % 128
        place = index // 128
        for half in range(own // 8):
            at = pl.ds(8 * half, 8)
            total = jnp.zeros((8, nobs), jnp.float32)
            for g in range(cells // 128):
                found = jnp.take_along_axis(
                    packed[b, at, pl.ds(128 * g, 128)], lane, axis=1, mode="promise_in_bounds"
                )
                total = jnp.where(place == ORDER[g], found, total)
            picked[b + 1, at, :] = total
        return carry

    lax.fori_loop(0, parts, pick, 0, unroll=8)
    picked[0] = picked[parts]
    picked[parts + 1] = picked[1]

    start_all(seen_copy)
    for role in range(3):
        seen[role, mine, :] = picked[me + role]
    members[mine, :] = packed[me]
    seen_all.wait_recv()
    for c in range(EARLY, len(PIECES)):
        start_all(patch_copy(c))

    row_id = lax.broadcasted_iota(jnp.int32, (size, size), 0)
    column_id = lax.broadcasted_iota(jnp.int32, (size, size), 1)
    diagonal = row_id == column_id
    gram = jnp.where(diagonal, size - 1.0, 0.0)
    pull = jnp.zeros((size, 1), jnp.float32)
    for role in range(3):
        patch = lax.rem(me + role + parts - 1, parts)
        value = obs_value[0, pl.ds(patch, 1), :]
        error = obs_error[0, pl.ds(patch, 1), :]
        level = loc_index[0, pl.ds(patch, 1), :]
        weight = jnp.zeros_like(value)
        for i in range(loc_table.shape[1]):
            weight = weight + jnp.where(level == i, loc_table[role, i], 0.0)
        precision = weight / error
        observed = seen[role]
        obs_mean = jnp.sum(observed, axis=0, keepdims=True) * (1.0 / size)
        spread = observed - obs_mean
        pull = pull + jnp.sum(
            spread * (precision * (value - obs_mean)), axis=1, keepdims=True
        )
        left_high, left_low = split(spread * precision)
        right_high, right_low = split(spread)
        gram = gram + sum(
            lax.dot_general(
                a, b, (((1,), (1,)), ((), ())), preferred_element_type=jnp.float32
            )
            for a, b in (
                (left_high, right_high),
                (left_high, right_low),
                (left_low, right_high),
                (left_low, right_low),
            )
        )
    square = jnp.sum(jnp.sum(gram * gram, axis=0, keepdims=True), axis=1, keepdims=True)
    inverse_scale = 1.0 / jnp.sqrt(square)

    def put(parts_ref, value):
        high, low = split(value)
        parts_ref[0] = high
        parts_ref[1] = low

    def product(a, b):
        return dot3(a[0], a[1], b[0], b[1])

    scaled = gram * inverse_scale
    put(matrix_parts, scaled)
    factor = jnp.where(diagonal, 1.5, 0.0) - 0.5 * scaled
    put(factor_parts, factor)
    put(root_parts, factor)
    put(matrix_parts, product(matrix_parts, factor_parts))

    def iterate(i, carry):
        put(
            factor_parts,
            jnp.where(diagonal, 1.5, 0.0) - 0.5 * product(root_parts, matrix_parts),
        )
        put(matrix_parts, product(matrix_parts, factor_parts))
        put(root_parts, product(factor_parts, root_parts))
        return carry

    lax.fori_loop(0, NS_ITERS - 2, iterate, 0)
    put(
        factor_parts,
        jnp.where(diagonal, 1.5, 0.0) - 0.5 * product(root_parts, matrix_parts),
    )
    root[...] = product(factor_parts, root_parts)

    pull_row = jnp.sum(jnp.where(diagonal, pull, 0.0), axis=0, keepdims=True)
    once = jnp.sum(root[...] * pull_row, axis=1, keepdims=True)
    mean_weight = jnp.sum(root[...] * once, axis=0, keepdims=True) * inverse_scale
    put(root_parts, jnp.sqrt((size - 1.0) * inverse_scale) * root[...] + mean_weight)

    for c, (first_block, last_block) in enumerate(PIECES):
        patch_all(c).wait_recv()
        for first in range(first_block, last_block, 2):
            many = min(2, last_block - first)
            lanes = pl.ds(128 * first, 128 * many)
            block = members[:, lanes]
            center = jnp.sum(block, axis=0, keepdims=True) * (1.0 / size)
            high, low = split(block - center)
            result[:, lanes] = center + dot3(root_parts[0], root_parts[1], high, low)
        start_all(back_copy(c))

    def unpack(place, g):
        lanes = pl.ds(128 * place, 128)
        for half in range(own // 8):
            at = pl.ds(8 * half, 8)
            for block in range(lane_tiles):
                values = [back[8 * block + p, at, lanes] for p in range(8)]
                for r, value in enumerate(exchange_groups(values, group)):
                    levels[0, 8 * g + r, at, pl.ds(128 * block, 128)] = value

    back[me] = result[mine, :]
    for copy in halo:
        copy.wait_send()
    stores = []
    for c, (first_block, last_block) in enumerate(PIECES):
        back_all(c).wait_recv()
        for place in range(first_block, last_block):
            g = ORDER[place]
            unpack(place, g)
            rows = pl.ds(8 * g, 8)
            for m in range(own):
                store = pltpu.make_async_copy(
                    levels.at[0, rows, m], out.at[m, rows], out_sem.at[g, m]
                )
                store.start()
                stores.append(store)
    seen_all.wait_send()
    patch_sent.wait_send()
    back_sent.wait_send()
    for store in stores:
        store.wait()


def body(*args, parts, tiles):
    field = args[0]
    own, _, width = field.shape
    size = own * parts
    cells = ROWS * COLS
    nobs = args[4].shape[2]
    f32 = jnp.float32
    dma = pltpu.SemaphoreType.DMA
    hbm = pl.BlockSpec(memory_space=pl.ANY)
    vmem = pl.BlockSpec(memory_space=pltpu.VMEM)
    smem = pl.BlockSpec(memory_space=pltpu.SMEM)
    tall = ROWS + 2 * PAD
    pair = pltpu.VMEM((2, size, size), jnp.bfloat16)
    return pl.pallas_call(
        functools.partial(main_kernel, parts=parts, tiles=tiles),
        out_shape=jax.ShapeDtypeStruct(field.shape, f32),
        in_specs=[hbm] * 4 + [vmem] * 4 + [smem],
        out_specs=hbm,
        scratch_shapes=[
            pltpu.VMEM((PASSES + 1, tall, own, width), f32),
            pltpu.VMEM((3, tall, width), f32),
            pltpu.VMEM((4, tall, 8, width), f32),
            pltpu.VMEM((parts, own, cells), f32),
            pltpu.VMEM((parts + 2, own, nobs), f32),
            pltpu.VMEM((size, cells), f32),
            pltpu.VMEM((3, size, nobs), f32),
            pltpu.VMEM((size, size), f32),
            pair,
            pair,
            pair,
            pltpu.VMEM((parts, own, cells), f32),
            pltpu.VMEM((size, cells), f32),
            dma((own + 3,)),
            dma((ROWS // 8, own)),
            pltpu.SemaphoreType.REGULAR((4,)),
            dma((4,)),
            dma((4,)),
            dma,
            dma,
            dma,
            dma((len(PIECES),)),
            dma,
            dma((len(PIECES),)),
        ],
        compiler_params=pltpu.CompilerParams(
            collective_id=0, has_side_effects=True, vmem_limit_bytes=VMEM_LIMIT
        ),
        name="forecast_and_analysis",
    )(*args)


def solution(mesh):
    parts, tiles = mesh.shape["mem"], mesh.shape["tile"]
    in_specs = (
        P("mem", "tile", None),
        P("tile", None),
        P("tile", None),
        P("tile", None),
        P("tile", None, None),
        P("tile", None, None),
        P("tile", None, None),
        P("tile", None, None),
        P(),
    )
    return jax.shard_map(
        functools.partial(body, parts=parts, tiles=tiles),
        mesh=mesh,
        in_specs=in_specs,
        out_specs=P("mem", "tile", None),
        check_vma=False,
    )
```
